256 devices in a mesh: dp: 8 (over z), expert: 32 (over x, y, core).
Axes of the slice: x: 4, y: 4, z: 8, core: 2. Of those that a mesh axis runs over, the one named last changes fastest.
Arguments:
- tokens: bfloat16 [2048, 7168], P('expert'), may hold values from -6 to 6
- routes: int32 [2048, 8], P('expert'), may hold values from 0 to 31, all different within a row; in each aligned block of 64 rows (0 to 63, 64 to 127, ...) at most 20 rows name the same one
- route_weight: int32 [2048, 8], P('expert'), may hold values from 1 to 4096
- w_gate: bfloat16 [32, 7168, 2048], P('expert', None, 'dp'), may hold values from -0.0625 to 0.0625
- w_up: bfloat16 [32, 7168, 2048], P('expert', None, 'dp'), may hold values from -0.0625 to 0.0625
- w_down: bfloat16 [32, 2048, 7168], P('expert', 'dp'), may hold values from -0.125 to 0.125
- prev_inputs: bfloat16 [8, 32, 64, 7168], P('dp', 'expert'), may hold values from -6 to 6
Outputs:
- mixed: bfloat16 [2048, 7168], P('expert', 'dp')
- hessian: float32 [7168, 32, 128], P('dp', 'expert')
The draws below stay inside these ranges and needn't reach their ends.
Inputs may be any that keep to these rules, and one draw needn't show every extreme that they name: `routes`: in each aligned block of 64 rows (the rows of one index of expert) no expert is named more than 20 times, a bound that some block reaches; the 8 experts of a token differ.
All inputs are finite; a program needn't handle non-finite values.
Results may differ from the reference program's by a relative error of at most 0.014.
Values may be sent and summed in bfloat16 or wider, within the bound.
A program may use at most 128 MiB of HBM per device.

```python
import math
import jax
import jax.numpy as jnp
import numpy as np
from jax import lax

D = 7168
FF = 2048
TOP = 8
TOK_DEV = 64
PREV_ROWS = 64
HESS_COLS = 128
EXPERTS = 32
TOKENS = 2048
CAP = 20
N_DP = 8
N_EXPERT = 32


def with_ends(result, rng, smallest, largest):
    shape = result.shape
    spot = [jax.random.randint(jax.random.fold_in(rng, axis), (), 0, shape[axis]) for axis in range(len(shape))]
    result = result.at[tuple(spot)].set(smallest)
    longest = shape.index(max(shape))
    spot[longest] = (spot[longest] + 1) % shape[longest]
    return result.at[tuple(spot)].set(largest)


def block_scale(rng, extent, pieces, low, top_value):
    def one(position, blocks):
        steps = jax.random.uniform(jax.random.fold_in(jax.random.fold_in(rng, 6), position), (blocks,), jnp.float32, low / len(pieces), top_value / len(pieces))
        return jnp.repeat(jnp.exp(steps), extent[position] // blocks).reshape((-1,) + (1,) * (len(extent) - position - 1))

    level = one(*pieces[0])
    for cut in pieces[1:]:
        level = level * one(*cut)
    return level


def shared_out(own_key, own, number, rows, number_of, top, bound, skew):
    order = jax.random.permutation(own_key, number_of)
    crowded, usual = load_shares(number_of, rows * top, bound, skew, True), load_shares(number_of, rows * top, bound, skew, False)
    places = jnp.arange(number_of)

    def named(lengths, offset_by):
        used = int((lengths > 0).sum())
        fixed = max(1, used // 4)
        moved = fixed + (places - fixed + offset_by * (used - fixed)) % max(1, number_of - fixed)
        return jnp.zeros((number_of,), jnp.int32).at[order[jnp.where(places < fixed, places, moved)]].set(jnp.asarray(lengths, jnp.int32))

    lengths = jnp.where(number % 4 == 0, named(crowded, number // 4), named(usual, number - number // 4 - 1))
    mixed = jax.random.permutation(jax.random.fold_in(own, 3), number_of)
    giver, sink = mixed[0:number_of // 2 * 2:2], mixed[1:number_of // 2 * 2:2]
    margin = jnp.minimum(lengths[giver] - 1, bound - lengths[sink]) // 2
    margin = jnp.where((giver == order[0]) | (sink == order[0]) | (lengths[sink] == 0), 0, jnp.maximum(margin, 0))
    moved = jax.random.randint(jax.random.fold_in(own, 4), (number_of // 2,), 0, 1 << 20) % (margin + 1)
    lengths = lengths.at[giver].add(-moved).at[sink].add(moved)
    labels = jnp.searchsorted(jnp.cumsum(lengths), jnp.arange(rows * top), side="right").astype(jnp.int32)
    listing = labels.reshape(top, rows).T
    listing = listing[jax.random.permutation(jax.random.fold_in(own, 1), rows)]
    offset_by = jax.random.randint(jax.random.fold_in(own, 2), (rows, 1), 0, top)
    return jnp.take_along_axis(listing, (jnp.arange(top)[None, :] + offset_by) % top, axis=1)


def load_shares(amount, total, reach, lean, full):
    portions = [(1 << 20) // math.isqrt(grade ** lean) + 1 for grade in range(1, amount + 1)]
    largest = reach if full else min(reach, max(-(-total // amount), total * portions[0] // sum(portions)))
    least = 1 if total - largest >= amount - 1 else 0
    holding, surplus = [largest] + [least] * (amount - 1), total - largest - least * (amount - 1)
    while surplus > 0:
        candidates = [i for i in range(1, amount) if holding[i] < largest] or [i for i in range(1, amount) if holding[i] < reach]
        pool, budget = sum([portions[i] for i in candidates]), surplus
        for i in candidates:
            addition = min(reach - holding[i], max(1, budget * portions[i] // pool), surplus)
            holding[i] = holding[i] + addition
            surplus = surplus - addition
    return np.array(holding)


def centred(key, extent, width, most, shards=(), held_as=jnp.bfloat16):
    gain = block_scale(key, extent, shards, -0.22, 0.18) if shards else 1.0
    values = jax.random.normal(key, extent, jnp.float32) * width * gain
    return jnp.minimum(jnp.maximum(values, -most), most).astype(held_as)


def setup_inputs(seed: int = 0) -> dict:
    keys = jax.random.split(jax.random.key(seed), 8)
    tokens = centred(keys[0], (TOKENS, D), 1.0, 6.0, ((0, 32),))
    routes_keys = jax.random.split(jax.random.fold_in(keys[1], 1), TOKENS // TOK_DEV)
    routes_turns = jax.random.permutation(jax.random.fold_in(keys[1], 3), TOKENS // TOK_DEV)
    routes = jax.vmap(lambda own, number: shared_out(jax.random.fold_in(keys[1], 2), own, number, TOK_DEV, EXPERTS, TOP, CAP, 2))(routes_keys, routes_turns).reshape((TOKENS, TOP))
    route_weight = with_ends(jax.random.randint(keys[2], (TOKENS, TOP), 1, 4097), jax.random.fold_in(keys[2], 1), 1, 4096).astype(jnp.int32)
    w_gate = centred(keys[3], (EXPERTS, D, FF), D ** -0.5, 0.0625, ((0, 32), (2, 8)))
    w_up = centred(keys[4], (EXPERTS, D, FF), D ** -0.5, 0.0625, ((0, 32), (2, 8)))
    w_down = centred(keys[5], (EXPERTS, FF, D), FF ** -0.5, 0.125, ((0, 32), (1, 8)))
    prev_inputs = centred(keys[6], (N_DP, EXPERTS, PREV_ROWS, D), 1.0, 6.0, ((0, 8), (1, 32)))
    return {"tokens": tokens, "routes": routes, "route_weight": route_weight, "w_gate": w_gate, "w_up": w_up, "w_down": w_down, "prev_inputs": prev_inputs}


def route_slots(flat_ids):
    onehot = (flat_ids[:, None] == jnp.arange(EXPERTS, dtype=jnp.int32)[None, :]).astype(jnp.int32)
    earlier = jnp.cumsum(onehot, axis=0) - onehot
    return jnp.sum(earlier * onehot, axis=1).astype(jnp.int32)


def reference(tokens, routes, route_weight, w_gate, w_up, w_down, prev_inputs):
    blocks = routes.reshape(N_EXPERT, TOK_DEV * TOP).astype(jnp.int32)
    slots = jax.vmap(route_slots)(blocks)
    anchor = jnp.arange(N_EXPERT, dtype=jnp.int32)[:, None]
    places = ((blocks * N_EXPERT + anchor) * CAP + slots).astype(jnp.int32)
    token_ids = jnp.arange(TOKENS, dtype=jnp.int32).reshape(N_EXPERT, TOK_DEV, 1)
    token_ids = jnp.broadcast_to(token_ids, (N_EXPERT, TOK_DEV, TOP)).reshape(N_EXPERT, TOK_DEV * TOP)
    table = jnp.full((EXPERTS * N_EXPERT * CAP,), TOKENS, jnp.int32)
    table = table.at[places.reshape(-1)].set(token_ids.reshape(-1)).reshape(EXPERTS, N_EXPERT * CAP)
    padded = jnp.concatenate([tokens, jnp.zeros((1, D), tokens.dtype)], axis=0)
    slice_width = FF // N_DP

    def one_expert(item):
        index, gate_w, up_w, down_w = item
        rows = padded[index]
        gate = jnp.dot(rows, gate_w, preferred_element_type=jnp.float32)
        up = jnp.dot(rows, up_w, preferred_element_type=jnp.float32)
        hidden = (jax.nn.silu(gate) * up).astype(jnp.bfloat16)
        total = jnp.zeros((N_EXPERT * CAP, D), jnp.float32)
        for group in range(N_DP):
            piece = jnp.dot(hidden[:, group * slice_width:(group + 1) * slice_width],
                            down_w[group * slice_width:(group + 1) * slice_width],
                            preferred_element_type=jnp.float32).astype(jnp.bfloat16)
            total = total + lax.optimization_barrier(piece).astype(jnp.float32)
        return total

    outputs = lax.map(one_expert, (table, w_gate, w_up, w_down))
    flat_out = outputs.reshape(EXPERTS * N_EXPERT * CAP, D)
    picked = flat_out[places.reshape(-1)].reshape(TOKENS, TOP, D)
    counts = route_weight.astype(jnp.float32)
    shares = 2.5 * counts / jnp.sum(counts, axis=1, keepdims=True)
    mixed = jnp.sum(picked * shares[:, :, None], axis=1).astype(jnp.bfloat16)

    def one_gram(history):
        rows = history.reshape(N_DP * PREV_ROWS, D)
        gram = jnp.dot(rows.T, rows[:, :HESS_COLS], preferred_element_type=jnp.float32)
        return gram * (2.0 / (N_DP * PREV_ROWS))

    grams = lax.map(one_gram, jnp.moveaxis(prev_inputs, 1, 0))
    hessian = jnp.transpose(grams, (1, 0, 2))
    return mixed, hessian
```

```python
import functools

import jax
import jax.numpy as jnp
from jax import lax
from jax.experimental import pallas as pl
from jax.experimental.pallas import tpu as pltpu
from jax.sharding import PartitionSpec as P

HESS_COLS = 128
PARTS = 2
BOTH = ("dp", "expert")


def experts_kernel(groups, t_ref, wg_ref, wu_ref, wd_ref, share_ref, out_ref, gate, up, hidden):
    step = pl.program_id(0)

    @pl.when(step < groups)
    def _():
        rows = t_ref[0]
        more_gate = jnp.dot(rows, wg_ref[...], preferred_element_type=jnp.float32)
        more_up = jnp.dot(rows, wu_ref[...], preferred_element_type=jnp.float32)

        @pl.when(step == 0)
        def _():
            gate[...] = more_gate
            up[...] = more_up

        @pl.when(step > 0)
        def _():
            gate[...] += more_gate
            up[...] += more_up

    @pl.when(step == groups - 1)
    def _():
        value = gate[...]
        hidden[...] = (value / (1.0 + jnp.exp(-value)) * up[...]).astype(jnp.bfloat16)

    @pl.when(step >= groups)
    def _():
        part = jnp.dot(hidden[...], wd_ref[...], preferred_element_type=jnp.float32)
        part = part.astype(jnp.bfloat16).astype(jnp.float32)
        out_ref[...] = (part * share_ref[...]).astype(jnp.bfloat16)


def experts(gathered, w_gate, w_up, w_down, share):
    groups, rows, cols = gathered.shape
    ff = w_gate.shape[1]
    first = lambda i: jnp.minimum(i, groups - 1)
    second = lambda i: jnp.maximum(i - groups, 0)
    return pl.pallas_call(
        functools.partial(experts_kernel, groups),
        grid=(2 * groups,),
        out_shape=jax.ShapeDtypeStruct((rows, groups * cols), jnp.bfloat16),
        in_specs=[
            pl.BlockSpec((1, rows, cols), lambda i: (first(i), 0, 0)),
            pl.BlockSpec((cols, ff), lambda i: (first(i), 0)),
            pl.BlockSpec((cols, ff), lambda i: (first(i), 0)),
            pl.BlockSpec((ff, cols), lambda i: (0, second(i))),
            pl.BlockSpec((rows, 1), lambda i: (0, 0)),
        ],
        out_specs=pl.BlockSpec((rows, cols), lambda i: (0, second(i))),
        scratch_shapes=[
            pltpu.VMEM((rows, ff), jnp.float32),
            pltpu.VMEM((rows, ff), jnp.float32),
            pltpu.VMEM((rows, ff), jnp.bfloat16),
        ],
        compiler_params=pltpu.CompilerParams(
            dimension_semantics=("arbitrary",), vmem_limit_bytes=48 * 2**20
        ),
        cost_estimate=pl.CostEstimate(
            flops=6 * rows * groups * cols * ff,
            bytes_accessed=2 * (2 * groups * rows * cols + 3 * groups * cols * ff),
            transcendentals=rows * ff,
        ),
    )(gathered, w_gate, w_up, w_down, share)


def shards(tokens, routes, route_weight, w_gate, w_up, w_down, prev_inputs):
    tok_dev, top = routes.shape
    width = tokens.shape[1]
    n_expert = lax.axis_size("expert")
    n_dp = lax.axis_size("dp")
    col_width = width // n_dp
    tok_part = tok_dev // PARTS
    my_cols = lax.dynamic_slice_in_dim(tokens, lax.axis_index("dp") * col_width, col_width, 1)
    gathered = []
    for p in range(PARTS):
        block = my_cols[p * tok_part : (p + 1) * tok_part]
        whole = lax.all_gather(block, BOTH, axis=0, tiled=False)
        gathered.append(whole.reshape(n_dp, n_expert * tok_part, col_width))

    weight_counts = route_weight.astype(jnp.float32)
    shares = 2.5 * weight_counts / jnp.sum(weight_counts, axis=1, keepdims=True)
    named = jnp.arange(n_expert, dtype=jnp.int32)[:, None, None] == routes[None]
    by_expert = jnp.sum(jnp.where(named, shares[None], 0.0), axis=2)
    mine = lax.all_to_all(by_expert, "expert", split_axis=0, concat_axis=0, tiled=True)

    history = prev_inputs.reshape(prev_inputs.shape[2], width)
    head = lax.all_gather(history[:, :HESS_COLS], "dp", axis=0, tiled=True)
    pieces = jnp.moveaxis(history.reshape(-1, n_dp, col_width), 1, 0)
    pieces = lax.all_to_all(pieces, "dp", split_axis=0, concat_axis=0, tiled=True)
    stacked = pieces.reshape(-1, col_width)
    hessian = jnp.einsum("rd,rh->dh", stacked, head, preferred_element_type=jnp.float32)
    hessian = (hessian * (2.0 / stacked.shape[0]))[:, None, :]

    mixed = []
    for p in range(PARTS):
        share = mine[:, p * tok_part : (p + 1) * tok_part].reshape(-1, 1)
        out = experts(gathered[p], w_gate[0], w_up[0], w_down[0], share)
        own = lax.psum_scatter(out, "expert", scatter_dimension=0, tiled=True)
        own = jnp.moveaxis(own.reshape(tok_part, n_dp, col_width), 1, 0)
        mixed.append(lax.psum_scatter(own, "dp", scatter_dimension=0, tiled=True)[0])
    return (jnp.concatenate(mixed, axis=0), hessian)


def solution(mesh):
    placed = (
        P("expert", None),
        P("expert", None),
        P("expert", None),
        P("expert", None, "dp"),
        P("expert", None, "dp"),
        P("expert", "dp", None),
        P("dp", "expert", None, None),
    )
    return jax.shard_map(
        shards,
        mesh=mesh,
        in_specs=placed,
        out_specs=(P("expert", "dp"), P("dp", "expert", None)),
        check_vma=False,
    )
```

```python
import functools

import jax
import jax.numpy as jnp
from jax import lax
from jax.experimental import pallas as pl
from jax.experimental.pallas import tpu as pltpu
from jax.sharding import PartitionSpec as P

HESS_COLS = 128
SIDE = 4
CHIPS = SIDE * SIDE
UNITS = 56
SWAP_UNITS = 18
MESH = pl.DeviceIdType.MESH
BF16 = jnp.bfloat16
F32 = jnp.float32


class Place:
    def __init__(self):
        self.n_dp = lax.axis_size("dp")
        self.z = lax.axis_index("dp")
        e = lax.axis_index("expert")
        self.core = lax.rem(e, 2)
        chip = e // 2
        self.y = lax.rem(chip, SIDE)
        self.x = chip // SIDE

    def block(self, axis, first, second):
        dx, dy = (first, second) if axis == "x" else (second, first)
        return lax.rem(self.x + dx + SIDE, SIDE) * SIDE + lax.rem(self.y + dy + SIDE, SIDE)

    def device(self, dx=0, dy=0, dz=0):
        chip = self.block("x", dx, dy)
        return (lax.rem(self.z + dz + self.n_dp, self.n_dp), chip * 2 + self.core)

    def toward(self, axis, step):
        return self.device(dx=step) if axis == "x" else self.device(dy=step)

    def partner(self):
        chip = self.block("x", 0, 0)
        return (self.z, chip * 2 + 1 - self.core)


def greet(devices):
    barrier = pltpu.get_barrier_semaphore()
    for device in devices:
        pl.semaphore_signal(barrier, inc=1, device_id=device, device_id_type=MESH)
    pl.semaphore_wait(barrier, len(devices))


def remote(src, dst, send_sem, recv_sem, device):
    return pltpu.make_async_remote_copy(
        src_ref=src,
        dst_ref=dst,
        send_sem=send_sem,
        recv_sem=recv_sem,
        device_id=device,
        device_id_type=MESH,
    )


def take_turns(flows):
    flows = list(flows)
    while flows:
        left = []
        for flow in flows:
            try:
                next(flow)
                left.append(flow)
            except StopIteration:
                pass
        flows = left


def gather_kernel(
    tok_ref, share_ref, wg_ref, wu_ref, wd_ref,
    all_ref, shares_ref, wg2_ref, wu2_ref, wd2_ref,
    flow_send, flow_recv, z_send, z_recv, s_send, s_recv, w_send, w_recv, local_sem,
):
    here = Place()
    width = tok_ref.shape[1]
    unit = width // UNITS
    offsets = [(i, j) for i in range(SIDE) for j in range(SIDE) if (i, j) != (0, 0)]
    z_steps = (1, -1)
    greet([here.device(dx=i, dy=j) for i, j in offsets]
          + [here.device(dz=s) for s in z_steps] + [here.partner()])
    own = here.block("x", 0, 0)
    started = []

    def go(copy):
        copy.start()
        started.append(copy)
        return copy

    parity = lax.rem(here.z, 2)
    swap = SWAP_UNITS * unit
    swap_from = pl.multiple_of((1 - parity) * swap, unit)
    wanted_from = pl.multiple_of(parity * swap, unit)

    def flow(number, axis, other, start, span, swapped):
        half = span // 2
        whole = pl.ds(start, span)
        part_a, part_b = pl.ds(start, half), pl.ds(pl.multiple_of(start + half, unit), half)

        def send(t, rel, cols, along, step, local=False):
            block = here.block(axis, *rel)
            src = tok_ref.at[:, cols] if local else all_ref.at[block, :, cols]
            return go(remote(src, all_ref.at[block, :, cols], flow_send.at[number, t],
                             flow_recv.at[number, t], here.toward(along, step)))

        def across(rel, which):
            if not swapped:
                return
            block = here.block(axis, *rel)
            slot = (rel[0] % SIDE) * SIDE + rel[1] % SIDE
            for side in which:
                cols = (part_a, part_b)[side]
                ref = all_ref.at[block, :, cols]
                go(remote(ref, ref, z_send.at[side, slot], z_recv.at[side, slot],
                          here.device(dz=z_steps[side])))

        c = {}
        c[0] = send(0, (0, 0), whole, axis, 1, True)
        c[1] = send(1, (0, 0), whole, axis, -1, True)
        c[2] = send(2, (0, 0), whole, other, 1, True)
        c[3] = send(3, (0, 0), whole, other, -1, True)
        yield
        c[0].wait_recv()
        c[4] = send(4, (-1, 0), part_a, axis, 1)
        c[5] = send(5, (-1, 0), whole, other, 1)
        c[6] = send(6, (-1, 0), whole, other, -1)
        across((-1, 0), (0, 1))
        c[1].wait_recv()
        c[7] = send(7, (1, 0), part_b, axis, -1)
        c[8] = send(8, (1, 0), whole, other, 1)
        c[9] = send(9, (1, 0), whole, other, -1)
        across((1, 0), (0, 1))
        yield
        c[2].wait_recv()
        c[10] = send(10, (0, -1), part_a, other, 1)
        across((0, -1), (0, 1))
        c[3].wait_recv()
        c[11] = send(11, (0, 1), part_b, other, -1)
        across((0, 1), (0, 1))
        yield
        c[4].wait_recv()
        across((2, 0), (0,))
        c[7].wait_recv()
        across((2, 0), (1,))
        c[12] = send(12, (2, 0), whole, other, 1)
        c[13] = send(13, (2, 0), whole, other, -1)
        yield
        c[5].wait_recv()
        c[14] = send(14, (-1, -1), part_a, other, 1)
        across((-1, -1), (0, 1))
        c[6].wait_recv()
        c[15] = send(15, (-1, 1), part_b, other, -1)
        across((-1, 1), (0, 1))
        yield
        c[8].wait_recv()
        c[16] = send(16, (1, -1), part_a, other, 1)
        across((1, -1), (0, 1))
        c[9].wait_recv()
        c[17] = send(17, (1, 1), part_b, other, -1)
        across((1, 1), (0, 1))
        yield
        c[10].wait_recv()
        across((0, 2), (0,))
        c[11].wait_recv()
        across((0, 2), (1,))
        yield
        c[12].wait_recv()
        c[18] = send(18, (2, -1), part_a, other, 1)
        across((2, -1), (0, 1))
        c[13].wait_recv()
        c[19] = send(19, (2, 1), part_b, other, -1)
        across((2, 1), (0, 1))
        yield
        for t, rel, side in ((14, (-1, 2), 0), (15, (-1, 2), 1), (16, (1, 2), 0), (17, (1, 2), 1),
                             (18, (2, 2), 0), (19, (2, 2), 1)):
            c[t].wait_recv()
            across(rel, (side,))
        yield

    def extras():
        mine = pltpu.make_async_copy(tok_ref, all_ref.at[own], local_sem)
        mine.start()
        yield
        gifts = []
        for n, (i, j) in enumerate(offsets):
            gifts.append(go(remote(share_ref.at[here.block("x", i, j)], shares_ref.at[own],
                                   s_send.at[n], s_recv.at[n], here.device(dx=i, dy=j))))
        for n, (src, dst) in enumerate(((wg_ref, wg2_ref), (wu_ref, wu2_ref), (wd_ref, wd2_ref))):
            gifts.append(go(remote(src, dst, w_send.at[n], w_recv.at[n], here.partner())))
        shares_ref[own] = share_ref[own]
        for _ in range(6):
            yield
        for gift in gifts:
            gift.wait_recv()
        mine.wait()

    fixed = 2 * swap
    take_turns([
        flow(0, "x", "y", fixed, width - fixed, False),
        flow(1, "y", "x", swap_from, swap, True),
        extras(),
    ])
    half = swap // 2
    for side in (0, 1):
        cols = pl.ds(pl.multiple_of(wanted_from + side * half, unit), half)
        for i, j in offsets:
            ref = all_ref.at[here.block("y", i, j), :, cols]
            slot = i * SIDE + j
            remote(ref, ref, z_send.at[side, slot], z_recv.at[side, slot],
                   here.device(dz=z_steps[side])).wait_recv()
    for copy in started:
        copy.wait_send()


def gather_all(tokens, share, w_gate, w_up, w_down):
    rows, width = tokens.shape
    vmem, hbm = pl.BlockSpec(memory_space=pltpu.VMEM), pl.BlockSpec(memory_space=pl.ANY)
    dma = pltpu.SemaphoreType.DMA
    like = lambda a: jax.ShapeDtypeStruct(a.shape, a.dtype)
    return pl.pallas_call(
        gather_kernel,
        out_shape=[
            jax.ShapeDtypeStruct((CHIPS, rows, width), BF16),
            like(share), like(w_gate), like(w_up), like(w_down),
        ],
        in_specs=[vmem, vmem, hbm, hbm, hbm],
        out_specs=[hbm, vmem, hbm, hbm, hbm],
        scratch_shapes=[
            dma((2, 20)), dma((2, 20)), dma((2, CHIPS)), dma((2, CHIPS)),
            dma((CHIPS - 1,)), dma((CHIPS - 1,)), dma((3,)), dma((3,)), dma(()),
        ],
        compiler_params=pltpu.CompilerParams(
            collective_id=0, has_side_effects=True, vmem_limit_bytes=60 * 2**20
        ),
    )(tokens, share, w_gate, w_up, w_down)


def experts_kernel(
    steps, t_ref, ga_ref, ua_ref, gb_ref, ub_ref, da_ref, db_ref, share_ref, out_ref,
    sums, hidden,
):
    step = pl.program_id(0)

    @pl.when(step < steps)
    def _():
        rows = t_ref[...]
        for n, w_ref in enumerate((ga_ref, ua_ref, gb_ref, ub_ref)):
            more = jnp.dot(rows, w_ref[...], preferred_element_type=F32)

            @pl.when(step == 0)
            def _():
                sums[n] = more

            @pl.when(step > 0)
            def _():
                sums[n] += more

    @pl.when(step == steps - 1)
    def _():
        for n in range(2):
            gate = sums[2 * n]
            value = gate / (1.0 + jnp.exp(-gate)) * sums[2 * n + 1]
            hidden[n] = (value * share_ref[:, n : n + 1]).astype(BF16)

    @pl.when(step >= steps)
    def _():
        total = jnp.dot(hidden[0], da_ref[...], preferred_element_type=F32)
        total += jnp.dot(hidden[1], db_ref[...], preferred_element_type=F32)
        out_ref[...] = total.astype(BF16)


def experts(rows_all, own, other, share):
    rows, width = rows_all.shape
    ff = own[0].shape[1]
    steps = max(1, width // 1024)
    cols = width // steps
    first = lambda i: jnp.minimum(i, steps - 1)
    second = lambda i: jnp.maximum(i - steps, 0)
    up_spec = pl.BlockSpec((cols, ff), lambda i: (first(i), 0))
    down_spec = pl.BlockSpec((ff, cols), lambda i: (0, second(i)))
    return pl.pallas_call(
        functools.partial(experts_kernel, steps),
        grid=(2 * steps,),
        out_shape=jax.ShapeDtypeStruct((rows, width), BF16),
        in_specs=[
            pl.BlockSpec((rows, cols), lambda i: (0, first(i))),
            up_spec, up_spec, up_spec, up_spec, down_spec, down_spec,
            pl.BlockSpec((rows, 2), lambda i: (0, 0)),
        ],
        out_specs=pl.BlockSpec((rows, cols), lambda i: (0, second(i))),
        scratch_shapes=[pltpu.VMEM((4, rows, ff), F32), pltpu.VMEM((2, rows, ff), BF16)],
        compiler_params=pltpu.CompilerParams(
            dimension_semantics=("arbitrary",), vmem_limit_bytes=56 * 2**20
        ),
        cost_estimate=pl.CostEstimate(
            flops=12 * rows * width * ff,
            bytes_accessed=4 * rows * width + 12 * width * ff,
            transcendentals=2 * rows * ff,
        ),
    )(rows_all, own[0], own[1], other[0], other[1], own[2], other[2], share)


def scatter_kernel(
    part_ref, out_ref, held, half_in, full_in, half_in2, full_in2, z_in,
    load_sem, send1, recv1, send2, recv2, z_send, z_recv,
):
    here = Place()
    width = held.shape[2]
    group = out_ref.shape[1]
    own = here.block("x", 0, 0)
    z_offsets = range(1, here.n_dp)
    greet([here.device(dx=1), here.device(dx=-1), here.device(dy=1), here.device(dy=-1)]
          + [here.device(dz=j) for j in z_offsets])
    started = []
    order = (2, 1, -1, 0)

    def go(copy):
        copy.start()
        started.append(copy)
        return copy

    def flow(number, axis, other, start, span):
        half = span // 2
        whole = pl.ds(start, span)
        parts = (pl.ds(start, half), pl.ds(start + half, half))
        steps = (1, -1)
        halves, loads = {}, {}
        for k, s in enumerate(order):
            block = here.block(axis, 2, s)
            for side in (0, 1):
                halves[k, side] = go(remote(
                    part_ref.at[block, :, parts[side]], half_in.at[number, side, k],
                    send1.at[number, 0, side, k], recv1.at[number, 0, side, k],
                    here.toward(axis, steps[side])))
        for a, first in enumerate((1, -1, 0)):
            for k, s in enumerate(order):
                block = here.block(axis, first, s)
                copy = pltpu.make_async_copy(
                    part_ref.at[block, :, whole], held.at[block, :, whole],
                    load_sem.at[number, a, k])
                copy.start()
                loads[a, k] = copy
        yield
        fulls = {}
        for k, s in enumerate(order):
            for side in (0, 1):
                block = here.block(axis, steps[side], s)
                loads[side, k].wait()
                halves[k, side].wait_recv()
                cols = parts[side]
                summed = held[block, :, cols].astype(F32) + half_in[number, side, k].astype(F32)
                held[block, :, cols] = summed.astype(BF16)
                fulls[k, side] = go(remote(
                    held.at[block, :, whole], full_in.at[number, side, k],
                    send1.at[number, 1, side, k], recv1.at[number, 1, side, k],
                    here.toward(axis, steps[side])))
            yield

        def settle(k):
            block = here.block(axis, 0, order[k])
            loads[2, k].wait()
            fulls[k, 0].wait_recv()
            fulls[k, 1].wait_recv()
            summed = held[block, :, whole].astype(F32) + full_in[number, 0, k].astype(F32)
            summed += full_in[number, 1, k].astype(F32)
            held[block, :, whole] = summed.astype(BF16)
            return block

        block = settle(0)
        last = []
        for side in (0, 1):
            last.append(go(remote(
                held.at[block, :, parts[side]], half_in2.at[number, side],
                send2.at[number, 0, side], recv2.at[number, 0, side],
                here.toward(other, steps[side]))))
        yield
        blocks = [settle(1), settle(2)]
        yield
        settle(3)
        yield
        finals = []
        for side in (0, 1):
            block, cols = blocks[side], parts[side]
            last[side].wait_recv()
            summed = held[block, :, cols].astype(F32) + half_in2[number, side].astype(F32)
            held[block, :, cols] = summed.astype(BF16)
            finals.append(go(remote(
                held.at[block, :, whole], full_in2.at[number, side],
                send2.at[number, 1, side], recv2.at[number, 1, side],
                here.toward(other, steps[side]))))
        yield
        finals[0].wait_recv()
        finals[1].wait_recv()
        summed = held[own, :, whole].astype(F32) + full_in2[number, 0].astype(F32)
        summed += full_in2[number, 1].astype(F32)
        held[own, :, whole] = summed.astype(BF16)
        yield

    take_turns([
        flow(0, "x", "y", 0, width // 2),
        flow(1, "y", "x", width // 2, width // 2),
    ])

    def group_of(z):
        return pl.ds(pl.multiple_of(z * group, group), group)

    last = []
    for j in z_offsets:
        target = lax.rem(here.z + j, here.n_dp)
        last.append(go(remote(
            held.at[own, :, group_of(target)], z_in.at[j - 1],
            z_send.at[j - 1], z_recv.at[j - 1], here.device(dz=j))))
    total = held[own, :, group_of(here.z)].astype(F32)
    for j, copy in zip(z_offsets, last):
        copy.wait_recv()
        total += z_in[j - 1].astype(F32)
    out_ref[...] = total.astype(BF16)
    for copy in started:
        copy.wait_send()


def scatter_all(parts, n_dp):
    blocks, rows, width = parts.shape
    half, quarter, group = width // 2, width // 4, width // n_dp
    dma, vmem = pltpu.SemaphoreType.DMA, pltpu.VMEM
    return pl.pallas_call(
        scatter_kernel,
        out_shape=jax.ShapeDtypeStruct((rows, group), BF16),
        in_specs=[pl.BlockSpec(memory_space=pl.ANY)],
        out_specs=pl.BlockSpec(memory_space=pltpu.VMEM),
        scratch_shapes=[
            vmem((blocks, rows, width), BF16),
            vmem((2, 2, SIDE, rows, quarter), BF16),
            vmem((2, 2, SIDE, rows, half), BF16),
            vmem((2, 2, rows, quarter), BF16),
            vmem((2, 2, rows, half), BF16),
            vmem((n_dp - 1, rows, group), BF16),
            dma((2, 3, SIDE)),
            dma((2, 2, 2, SIDE)), dma((2, 2, 2, SIDE)),
            dma((2, 2, 2)), dma((2, 2, 2)),
            dma((n_dp - 1,)), dma((n_dp - 1,)),
        ],
        compiler_params=pltpu.CompilerParams(
            collective_id=1, has_side_effects=True, vmem_limit_bytes=60 * 2**20
        ),
    )(parts)


def shards(tokens, routes, route_weight, w_gate, w_up, w_down, prev_inputs):
    tok_dev, top = routes.shape
    width = tokens.shape[1]
    n_expert = lax.axis_size("expert")
    n_dp = lax.axis_size("dp")
    col_width = width // n_dp
    counts = route_weight.astype(F32)
    shares = 2.5 * counts / jnp.sum(counts, axis=1, keepdims=True)
    named = jnp.arange(n_expert, dtype=jnp.int32)[:, None, None] == routes[None]
    by_expert = jnp.sum(jnp.where(named, shares[None], 0.0), axis=2)
    by_chip = jnp.broadcast_to(by_expert.reshape(CHIPS, 1, 2 * tok_dev), (CHIPS, 8, 2 * tok_dev))
    whole, arrived, *other = gather_all(tokens, by_chip, w_gate[0], w_up[0], w_down[0])

    history = prev_inputs.reshape(prev_inputs.shape[2], width)
    head = min(HESS_COLS, col_width)
    pieces = jnp.moveaxis(history.reshape(-1, n_dp, col_width), 1, 0)
    heads = jnp.broadcast_to(history[None, :, :head], (n_dp, history.shape[0], head))
    pieces = jnp.concatenate([pieces, heads], axis=2)
    pieces, whole = lax.optimization_barrier((pieces, whole))
    moved = lax.all_to_all(pieces, "dp", split_axis=0, concat_axis=0, tiled=True)

    pairs = arrived[:, 0, :].reshape(CHIPS, 2, tok_dev)
    core = lax.rem(lax.axis_index("expert"), 2)
    pairs = jnp.where(core == 0, pairs, pairs[:, ::-1])
    share = jnp.moveaxis(pairs, 1, 2).reshape(CHIPS * tok_dev, 2)
    out = experts(whole.reshape(CHIPS * tok_dev, width), (w_gate[0], w_up[0], w_down[0]), other, share)
    out, moved = lax.optimization_barrier((out, moved))
    mixed = scatter_all(out.reshape(CHIPS, tok_dev, width), n_dp)

    stacked = moved.reshape(-1, col_width + head)
    hessian = jnp.einsum(
        "rd,rh->dh", stacked[:, :col_width], stacked[:, col_width:], preferred_element_type=F32
    )
    hessian = (hessian * (2.0 / stacked.shape[0]))[:, None, :]
    return (mixed, hessian)


def solution(mesh):
    placed = (
        P("expert", None),
        P("expert", None),
        P("expert", None),
        P("expert", None, "dp"),
        P("expert", None, "dp"),
        P("expert", "dp", None),
        P("dp", "expert", None, None),
    )
    return jax.shard_map(
        shards,
        mesh=mesh,
        in_specs=placed,
        out_specs=(P("expert", "dp"), P("dp", "expert", None)),
        check_vma=False,
    )
```

```python
import functools

import jax
import jax.numpy as jnp
from jax import lax
from jax.experimental import pallas as pl
from jax.experimental.pallas import tpu as pltpu
from jax.sharding import PartitionSpec as P

HESS_COLS = 128
SIDE = 4
CHIPS = SIDE * SIDE
UNITS = 56
SWAP_UNITS = 18
PARTS = 2
MESH = pl.DeviceIdType.MESH
BF16 = jnp.bfloat16
F32 = jnp.float32


class Place:
    def __init__(self):
        self.n_dp = lax.axis_size("dp")
        self.z = lax.axis_index("dp")
        e = lax.axis_index("expert")
        self.core = lax.rem(e, 2)
        chip = e // 2
        self.y = lax.rem(chip, SIDE)
        self.x = chip // SIDE

    def block(self, axis, first, second):
        dx, dy = (first, second) if axis == "x" else (second, first)
        return lax.rem(self.x + dx + SIDE, SIDE) * SIDE + lax.rem(self.y + dy + SIDE, SIDE)

    def device(self, dx=0, dy=0, dz=0):
        chip = self.block("x", dx, dy)
        return (lax.rem(self.z + dz + self.n_dp, self.n_dp), chip * 2 + self.core)

    def toward(self, axis, step):
        return self.device(dx=step) if axis == "x" else self.device(dy=step)

    def partner(self):
        chip = self.block("x", 0, 0)
        return (self.z, chip * 2 + 1 - self.core)


def greet(devices):
    barrier = pltpu.get_barrier_semaphore()
    for device in devices:
        pl.semaphore_signal(barrier, inc=1, device_id=device, device_id_type=MESH)
    pl.semaphore_wait(barrier, len(devices))


def remote(src, dst, send_sem, recv_sem, device):
    return pltpu.make_async_remote_copy(
        src_ref=src,
        dst_ref=dst,
        send_sem=send_sem,
        recv_sem=recv_sem,
        device_id=device,
        device_id_type=MESH,
    )


def take_turns(flows):
    flows = list(flows)
    while flows:
        left = []
        for flow in flows:
            try:
                next(flow)
                left.append(flow)
            except StopIteration:
                pass
        flows = left


def gather_kernel(
    tok_ref, share_ref, wg_ref, wu_ref, wd_ref,
    all_ref, shares_ref, wg2_ref, wu2_ref, wd2_ref,
    flow_send, flow_recv, z_send, z_recv, s_send, s_recv, w_send, w_recv, local_sem,
):
    here = Place()
    rows, width = tok_ref.shape
    unit = width // UNITS
    offsets = [(i, j) for i in range(SIDE) for j in range(SIDE) if (i, j) != (0, 0)]
    z_steps = (1, -1)
    greet([here.device(dx=i, dy=j) for i, j in offsets]
          + [here.device(dz=s) for s in z_steps] + [here.partner()])
    own = here.block("x", 0, 0)
    started = []

    def go(copy):
        copy.start()
        started.append(copy)
        return copy

    parity = lax.rem(here.z, 2)
    swap = SWAP_UNITS * unit
    swap_from = pl.multiple_of((1 - parity) * swap, unit)
    wanted_from = pl.multiple_of(parity * swap, unit)

    def flow(number, axis, other, start, span, swapped):
        half = span // 2
        band = pl.ds((number // 2) * (rows // PARTS), rows // PARTS)
        whole = pl.ds(start, span)
        part_a, part_b = pl.ds(start, half), pl.ds(pl.multiple_of(start + half, unit), half)

        def send(t, rel, cols, along, step, local=False):
            block = here.block(axis, *rel)
            src = tok_ref.at[band, cols] if local else all_ref.at[block, band, cols]
            return go(remote(src, all_ref.at[block, band, cols], flow_send.at[number, t],
                             flow_recv.at[number, t], here.toward(along, step)))

        def across(rel, which):
            if not swapped:
                return
            block = here.block(axis, *rel)
            slot = (rel[0] % SIDE) * SIDE + rel[1] % SIDE
            for side in which:
                cols = (part_a, part_b)[side]
                ref = all_ref.at[block, band, cols]
                part = number // 2
                go(remote(ref, ref, z_send.at[part, side, slot], z_recv.at[part, side, slot],
                          here.device(dz=z_steps[side])))

        c = {}
        c[0] = send(0, (0, 0), whole, axis, 1, True)
        c[1] = send(1, (0, 0), whole, axis, -1, True)
        c[2] = send(2, (0, 0), whole, other, 1, True)
        c[3] = send(3, (0, 0), whole, other, -1, True)
        yield
        c[0].wait_recv()
        c[4] = send(4, (-1, 0), part_a, axis, 1)
        c[5] = send(5, (-1, 0), whole, other, 1)
        c[6] = send(6, (-1, 0), whole, other, -1)
        across((-1, 0), (0, 1))
        c[1].wait_recv()
        c[7] = send(7, (1, 0), part_b, axis, -1)
        c[8] = send(8, (1, 0), whole, other, 1)
        c[9] = send(9, (1, 0), whole, other, -1)
        across((1, 0), (0, 1))
        yield
        c[2].wait_recv()
        c[10] = send(10, (0, -1), part_a, other, 1)
        across((0, -1), (0, 1))
        c[3].wait_recv()
        c[11] = send(11, (0, 1), part_b, other, -1)
        across((0, 1), (0, 1))
        yield
        c[4].wait_recv()
        across((2, 0), (0,))
        c[7].wait_recv()
        across((2, 0), (1,))
        c[12] = send(12, (2, 0), whole, other, 1)
        c[13] = send(13, (2, 0), whole, other, -1)
        yield
        c[5].wait_recv()
        c[14] = send(14, (-1, -1), part_a, other, 1)
        across((-1, -1), (0, 1))
        c[6].wait_recv()
        c[15] = send(15, (-1, 1), part_b, other, -1)
        across((-1, 1), (0, 1))
        yield
        c[8].wait_recv()
        c[16] = send(16, (1, -1), part_a, other, 1)
        across((1, -1), (0, 1))
        c[9].wait_recv()
        c[17] = send(17, (1, 1), part_b, other, -1)
        across((1, 1), (0, 1))
        yield
        c[10].wait_recv()
        across((0, 2), (0,))
        c[11].wait_recv()
        across((0, 2), (1,))
        yield
        c[12].wait_recv()
        c[18] = send(18, (2, -1), part_a, other, 1)
        across((2, -1), (0, 1))
        c[13].wait_recv()
        c[19] = send(19, (2, 1), part_b, other, -1)
        across((2, 1), (0, 1))
        yield
        for t, rel, side in ((14, (-1, 2), 0), (15, (-1, 2), 1), (16, (1, 2), 0), (17, (1, 2), 1),
                             (18, (2, 2), 0), (19, (2, 2), 1)):
            c[t].wait_recv()
            across(rel, (side,))
        yield

    def extras():
        mine = pltpu.make_async_copy(tok_ref, all_ref.at[own], local_sem)
        mine.start()
        yield
        gifts = []
        for n, (i, j) in enumerate(offsets):
            gifts.append(go(remote(share_ref.at[here.block("x", i, j)], shares_ref.at[own],
                                   s_send.at[n], s_recv.at[n], here.device(dx=i, dy=j))))
        shares_ref[own] = share_ref[own]
        for n, (src, dst) in enumerate(((wg_ref, wg2_ref), (wu_ref, wu2_ref), (wd_ref, wd2_ref))):
            gifts.append(go(remote(src, dst, w_send.at[n], w_recv.at[n], here.partner())))
            yield
        for _ in range(4):
            yield
        for gift in gifts:
            gift.wait_recv()
        mine.wait()

    fixed = 2 * swap
    flows = []
    for part in range(PARTS):
        flows.append(flow(2 * part, "x", "y", fixed, width - fixed, False))
        flows.append(flow(2 * part + 1, "y", "x", swap_from, swap, True))
    take_turns(flows + [extras()])
    half = swap // 2
    for part in range(PARTS):
        band = pl.ds(part * (rows // PARTS), rows // PARTS)
        for side in (0, 1):
            cols = pl.ds(pl.multiple_of(wanted_from + side * half, unit), half)
            for i, j in offsets:
                ref = all_ref.at[here.block("y", i, j), band, cols]
                slot = i * SIDE + j
                remote(ref, ref, z_send.at[part, side, slot], z_recv.at[part, side, slot],
                       here.device(dz=z_steps[side])).wait_recv()
    for copy in started:
        copy.wait_send()


def gather_all(tokens, share, w_gate, w_up, w_down):
    rows, width = tokens.shape
    vmem, hbm = pl.BlockSpec(memory_space=pltpu.VMEM), pl.BlockSpec(memory_space=pl.ANY)
    dma = pltpu.SemaphoreType.DMA
    like = lambda a: jax.ShapeDtypeStruct(a.shape, a.dtype)
    return pl.pallas_call(
        gather_kernel,
        out_shape=[
            jax.ShapeDtypeStruct((CHIPS, rows, width), BF16),
            like(share), like(w_gate), like(w_up), like(w_down),
        ],
        in_specs=[vmem, vmem, hbm, hbm, hbm],
        out_specs=[hbm, vmem, hbm, hbm, hbm],
        scratch_shapes=[
            dma((2 * PARTS, 20)), dma((2 * PARTS, 20)),
            dma((PARTS, 2, CHIPS)), dma((PARTS, 2, CHIPS)),
            dma((CHIPS - 1,)), dma((CHIPS - 1,)), dma((3,)), dma((3,)), dma(()),
        ],
        compiler_params=pltpu.CompilerParams(
            collective_id=0, has_side_effects=True, vmem_limit_bytes=60 * 2**20
        ),
    )(tokens, share, w_gate, w_up, w_down)


def experts_kernel(
    steps, t_ref, ga_ref, ua_ref, gb_ref, ub_ref, da_ref, db_ref, share_ref, out_ref,
    sums, hidden,
):
    step = pl.program_id(0)
    ff = ga_ref.shape[1]

    @pl.when(step < steps)
    def _():
        w = jnp.concatenate([ga_ref[...], ua_ref[...], gb_ref[...], ub_ref[...]], axis=1)
        more = jnp.dot(t_ref[...], w, preferred_element_type=F32)

        @pl.when(step == 0)
        def _():
            sums[...] = more

        @pl.when(step > 0)
        def _():
            sums[...] += more

    @pl.when(step == steps - 1)
    def _():
        for n in range(2):
            gate = sums[:, 2 * n * ff : (2 * n + 1) * ff]
            up = sums[:, (2 * n + 1) * ff : (2 * n + 2) * ff]
            value = gate / (1.0 + jnp.exp(-gate)) * up
            hidden[:, n * ff : (n + 1) * ff] = (value * share_ref[:, n : n + 1]).astype(BF16)

    @pl.when(step >= steps)
    def _():
        w = jnp.concatenate([da_ref[...], db_ref[...]], axis=0)
        out_ref[...] = jnp.dot(hidden[...], w, preferred_element_type=F32).astype(BF16)


def experts(rows_all, own, other, share):
    rows, width = rows_all.shape
    ff = own[0].shape[1]
    steps = max(1, width // 1792)
    cols = width // steps
    first = lambda i: jnp.minimum(i, steps - 1)
    second = lambda i: jnp.maximum(i - steps, 0)
    up_spec = pl.BlockSpec((cols, ff), lambda i: (first(i), 0))
    down_spec = pl.BlockSpec((ff, cols), lambda i: (0, second(i)))
    return pl.pallas_call(
        functools.partial(experts_kernel, steps),
        grid=(2 * steps,),
        out_shape=jax.ShapeDtypeStruct((rows, width), BF16),
        in_specs=[
            pl.BlockSpec((rows, cols), lambda i: (0, first(i))),
            up_spec, up_spec, up_spec, up_spec, down_spec, down_spec,
            pl.BlockSpec((rows, 2), lambda i: (0, 0)),
        ],
        out_specs=pl.BlockSpec((rows, cols), lambda i: (0, second(i))),
        scratch_shapes=[pltpu.VMEM((rows, 4 * ff), F32), pltpu.VMEM((rows, 2 * ff), BF16)],
        compiler_params=pltpu.CompilerParams(
            dimension_semantics=("arbitrary",), vmem_limit_bytes=58 * 2**20
        ),
        cost_estimate=pl.CostEstimate(
            flops=12 * rows * width * ff,
            bytes_accessed=4 * rows * width + 12 * width * ff,
            transcendentals=2 * rows * ff,
        ),
    )(rows_all, own[0], own[1], other[0], other[1], own[2], other[2], share)


def scatter_kernel(
    part_ref, out_ref, held, half_in, full_in, half_in2, full_in2, z_in,
    load_sem, send1, recv1, send2, recv2, z_send, z_recv,
):
    here = Place()
    rows, width = held.shape[1:]
    group = out_ref.shape[1]
    own = here.block("x", 0, 0)
    z_offsets = range(1, here.n_dp)
    greet([here.device(dx=1), here.device(dx=-1), here.device(dy=1), here.device(dy=-1)]
          + [here.device(dz=j) for j in z_offsets])
    started = []
    order = (2, 1, -1, 0)

    def go(copy):
        copy.start()
        started.append(copy)
        return copy

    def flow(number, axis, other, start, span):
        half = span // 2
        band = pl.ds((number // 2) * (rows // PARTS), rows // PARTS)
        whole = pl.ds(start, span)
        parts = (pl.ds(start, half), pl.ds(start + half, half))
        steps = (1, -1)
        halves, loads = {}, {}
        for k, s in enumerate(order):
            block = here.block(axis, 2, s)
            for side in (0, 1):
                halves[k, side] = go(remote(
                    part_ref.at[block, band, parts[side]], half_in.at[number, side, k],
                    send1.at[number, 0, side, k], recv1.at[number, 0, side, k],
                    here.toward(axis, steps[side])))
        for a, first in enumerate((1, -1, 0)):
            for k, s in enumerate(order):
                block = here.block(axis, first, s)
                copy = pltpu.make_async_copy(
                    part_ref.at[block, band, whole], held.at[block, band, whole],
                    load_sem.at[number, a, k])
                copy.start()
                loads[a, k] = copy
        yield
        fulls = {}
        for k, s in enumerate(order):
            for side in (0, 1):
                block = here.block(axis, steps[side], s)
                loads[side, k].wait()
                halves[k, side].wait_recv()
                cols = parts[side]
                summed = held[block, band, cols].astype(F32) + half_in[number, side, k].astype(F32)
                held[block, band, cols] = summed.astype(BF16)
                fulls[k, side] = go(remote(
                    held.at[block, band, whole], full_in.at[number, side, k],
                    send1.at[number, 1, side, k], recv1.at[number, 1, side, k],
                    here.toward(axis, steps[side])))
            yield

        def settle(k):
            block = here.block(axis, 0, order[k])
            loads[2, k].wait()
            fulls[k, 0].wait_recv()
            fulls[k, 1].wait_recv()
            summed = held[block, band, whole].astype(F32) + full_in[number, 0, k].astype(F32)
            summed += full_in[number, 1, k].astype(F32)
            held[block, band, whole] = summed.astype(BF16)
            return block

        block = settle(0)
        last = []
        for side in (0, 1):
            last.append(go(remote(
                held.at[block, band, parts[side]], half_in2.at[number, side],
                send2.at[number, 0, side], recv2.at[number, 0, side],
                here.toward(other, steps[side]))))
        yield
        blocks = [settle(1), settle(2)]
        yield
        settle(3)
        yield
        finals = []
        for side in (0, 1):
            block, cols = blocks[side], parts[side]
            last[side].wait_recv()
            summed = held[block, band, cols].astype(F32) + half_in2[number, side].astype(F32)
            held[block, band, cols] = summed.astype(BF16)
            finals.append(go(remote(
                held.at[block, band, whole], full_in2.at[number, side],
                send2.at[number, 1, side], recv2.at[number, 1, side],
                here.toward(other, steps[side]))))
        yield
        finals[0].wait_recv()
        finals[1].wait_recv()
        summed = held[own, band, whole].astype(F32) + full_in2[number, 0].astype(F32)
        summed += full_in2[number, 1].astype(F32)
        held[own, band, whole] = summed.astype(BF16)
        yield

    flows = []
    for part in range(PARTS):
        flows.append(flow(2 * part, "x", "y", 0, width // 2))
        flows.append(flow(2 * part + 1, "y", "x", width // 2, width // 2))

    def group_of(z):
        return pl.ds(pl.multiple_of(z * group, group), group)

    def spread(part):
        band = pl.ds(part * (rows // PARTS), rows // PARTS)
        copies = []
        for j in z_offsets:
            target = lax.rem(here.z + j, here.n_dp)
            copies.append(go(remote(
                held.at[own, band, group_of(target)], z_in.at[j - 1, band],
                z_send.at[part, j - 1], z_recv.at[part, j - 1], here.device(dz=j))))
        return copies

    def advance(part, count):
        for _ in range(count):
            for n in (2 * part, 2 * part + 1):
                next(flows[n])

    advance(0, 5)
    advance(1, 1)
    advance(0, 3)
    advance(1, 2)
    advance(0, 1)
    advance(1, 2)
    advance(0, 1)
    last = [spread(0)]
    advance(1, 5)
    last.append(spread(1))
    for part in range(PARTS):
        band = pl.ds(part * (rows // PARTS), rows // PARTS)
        total = held[own, band, group_of(here.z)].astype(F32)
        for j, copy in zip(z_offsets, last[part]):
            copy.wait_recv()
            total += z_in[j - 1, band].astype(F32)
        out_ref[band] = total.astype(BF16)
    for copy in started:
        copy.wait_send()


def scatter_all(parts, n_dp):
    blocks, rows, width = parts.shape
    half, quarter, group, band = width // 2, width // 4, width // n_dp, rows // PARTS
    dma, vmem = pltpu.SemaphoreType.DMA, pltpu.VMEM
    return pl.pallas_call(
        scatter_kernel,
        out_shape=jax.ShapeDtypeStruct((rows, group), BF16),
        in_specs=[pl.BlockSpec(memory_space=pl.ANY)],
        out_specs=pl.BlockSpec(memory_space=pltpu.VMEM),
        scratch_shapes=[
            vmem((blocks, rows, width), BF16),
            vmem((2 * PARTS, 2, SIDE, band, quarter), BF16),
            vmem((2 * PARTS, 2, SIDE, band, half), BF16),
            vmem((2 * PARTS, 2, band, quarter), BF16),
            vmem((2 * PARTS, 2, band, half), BF16),
            vmem((n_dp - 1, rows, group), BF16),
            dma((2 * PARTS, 3, SIDE)),
            dma((2 * PARTS, 2, 2, SIDE)), dma((2 * PARTS, 2, 2, SIDE)),
            dma((2 * PARTS, 2, 2)), dma((2 * PARTS, 2, 2)),
            dma((PARTS, n_dp - 1)), dma((PARTS, n_dp - 1)),
        ],
        compiler_params=pltpu.CompilerParams(
            collective_id=1, has_side_effects=True, vmem_limit_bytes=60 * 2**20
        ),
    )(parts)


def shards(tokens, routes, route_weight, w_gate, w_up, w_down, prev_inputs):
    tok_dev, top = routes.shape
    width = tokens.shape[1]
    n_expert = lax.axis_size("expert")
    n_dp = lax.axis_size("dp")
    col_width = width // n_dp
    counts = route_weight.astype(F32)
    shares = 2.5 * counts / jnp.sum(counts, axis=1, keepdims=True)
    named = jnp.arange(n_expert, dtype=jnp.int32)[:, None, None] == routes[None]
    by_expert = jnp.sum(jnp.where(named, shares[None], 0.0), axis=2)
    by_chip = jnp.broadcast_to(by_expert.reshape(CHIPS, 1, 2 * tok_dev), (CHIPS, 8, 2 * tok_dev))
    whole, arrived, *other = gather_all(tokens, by_chip, w_gate[0], w_up[0], w_down[0])

    history = prev_inputs.reshape(prev_inputs.shape[2], width)
    head = min(HESS_COLS, col_width)
    pieces = jnp.moveaxis(history.reshape(-1, n_dp, col_width), 1, 0)
    heads = jnp.broadcast_to(history[None, :, :head], (n_dp, history.shape[0], head))
    pieces = jnp.concatenate([pieces, heads], axis=2)
    pieces, whole = lax.optimization_barrier((pieces, whole))
    moved = lax.all_to_all(pieces, "dp", split_axis=0, concat_axis=0, tiled=True)

    pairs = arrived[:, 0, :].reshape(CHIPS, 2, tok_dev)
    core = lax.rem(lax.axis_index("expert"), 2)
    pairs = jnp.where(core == 0, pairs, pairs[:, ::-1])
    share = jnp.moveaxis(pairs, 1, 2).reshape(CHIPS * tok_dev, 2)
    out = experts(whole.reshape(CHIPS * tok_dev, width), (w_gate[0], w_up[0], w_down[0]), other, share)
    out, moved = lax.optimization_barrier((out, moved))
    mixed = scatter_all(out.reshape(CHIPS, tok_dev, width), n_dp)

    stacked = moved.reshape(-1, col_width + head)
    hessian = jnp.einsum(
        "rd,rh->dh", stacked[:, :col_width], stacked[:, col_width:], preferred_element_type=F32
    )
    hessian = (hessian * (2.0 / stacked.shape[0]))[:, None, :]
    return (mixed, hessian)


def solution(mesh):
    placed = (
        P("expert", None),
        P("expert", None),
        P("expert", None),
        P("expert", None, "dp"),
        P("expert", None, "dp"),
        P("expert", "dp", None),
        P("dp", "expert", None, None),
    )
    return jax.shard_map(
        shards,
        mesh=mesh,
        in_specs=placed,
        out_specs=(P("expert", "dp"), P("dp", "expert", None)),
        check_vma=False,
    )
```

```python
import functools

import jax
import jax.numpy as jnp
from jax import lax
from jax.experimental import pallas as pl
from jax.experimental.pallas import tpu as pltpu
from jax.sharding import PartitionSpec as P

HESS_COLS = 128
SIDE = 4
CHIPS = SIDE * SIDE
UNITS = 56
SWAP_UNITS = 18
PARTS = 2
BANDS = ((0, 48), (48, 16))
MESH = pl.DeviceIdType.MESH
BF16 = jnp.bfloat16
F32 = jnp.float32


class Place:
    def __init__(self):
        self.n_dp = lax.axis_size("dp")
        self.z = lax.axis_index("dp")
        e = lax.axis_index("expert")
        self.core = lax.rem(e, 2)
        chip = e // 2
        self.y = lax.rem(chip, SIDE)
        self.x = chip // SIDE

    def block(self, axis, first, second):
        dx, dy = (first, second) if axis == "x" else (second, first)
        return lax.rem(self.x + dx + SIDE, SIDE) * SIDE + lax.rem(self.y + dy + SIDE, SIDE)

    def device(self, dx=0, dy=0, dz=0):
        chip = self.block("x", dx, dy)
        return (lax.rem(self.z + dz + self.n_dp, self.n_dp), chip * 2 + self.core)

    def toward(self, axis, step):
        return self.device(dx=step) if axis == "x" else self.device(dy=step)

    def partner(self):
        chip = self.block("x", 0, 0)
        return (self.z, chip * 2 + 1 - self.core)


def greet(devices):
    barrier = pltpu.get_barrier_semaphore()
    for device in devices:
        pl.semaphore_signal(barrier, inc=1, device_id=device, device_id_type=MESH)
    pl.semaphore_wait(barrier, len(devices))


def remote(src, dst, send_sem, recv_sem, device):
    return pltpu.make_async_remote_copy(
        src_ref=src,
        dst_ref=dst,
        send_sem=send_sem,
        recv_sem=recv_sem,
        device_id=device,
        device_id_type=MESH,
    )


def take_turns(flows):
    flows = list(flows)
    while flows:
        left = []
        for flow in flows:
            try:
                next(flow)
                left.append(flow)
            except StopIteration:
                pass
        flows = left


def gather_kernel(
    tok_ref, share_ref, wg_ref, wu_ref, wd_ref,
    all_ref, shares_ref, wg2_ref, wu2_ref, wd2_ref,
    flow_send, flow_recv, z_send, z_recv, s_send, s_recv, w_send, w_recv, local_sem,
):
    here = Place()
    rows, width = tok_ref.shape
    unit = width // UNITS
    offsets = [(i, j) for i in range(SIDE) for j in range(SIDE) if (i, j) != (0, 0)]
    z_steps = (1, -1)
    greet([here.device(dx=i, dy=j) for i, j in offsets]
          + [here.device(dz=s) for s in z_steps] + [here.partner()])
    own = here.block("x", 0, 0)
    started = []

    def go(copy):
        copy.start()
        started.append(copy)
        return copy

    parity = lax.rem(here.z, 2)
    swap = SWAP_UNITS * unit
    swap_from = pl.multiple_of((1 - parity) * swap, unit)
    wanted_from = pl.multiple_of(parity * swap, unit)

    def flow(number, axis, other, start, span, swapped):
        half = span // 2
        band = pl.ds((number // 2) * (rows // PARTS), rows // PARTS)
        whole = pl.ds(start, span)
        part_a, part_b = pl.ds(start, half), pl.ds(pl.multiple_of(start + half, unit), half)

        def send(t, rel, cols, along, step, local=False):
            block = here.block(axis, *rel)
            src = tok_ref.at[band, cols] if local else all_ref.at[block, band, cols]
            return go(remote(src, all_ref.at[block, band, cols], flow_send.at[number, t],
                             flow_recv.at[number, t], here.toward(along, step)))

        def across(rel, which):
            if not swapped:
                return
            block = here.block(axis, *rel)
            slot = (rel[0] % SIDE) * SIDE + rel[1] % SIDE
            for side in which:
                cols = (part_a, part_b)[side]
                ref = all_ref.at[block, band, cols]
                part = number // 2
                go(remote(ref, ref, z_send.at[part, side, slot], z_recv.at[part, side, slot],
                          here.device(dz=z_steps[side])))

        c = {}
        c[0] = send(0, (0, 0), whole, axis, 1, True)
        c[1] = send(1, (0, 0), whole, axis, -1, True)
        yield
        c[2] = send(2, (0, 0), whole, other, 1, True)
        c[3] = send(3, (0, 0), whole, other, -1, True)
        yield
        c[0].wait_recv()
        c[4] = send(4, (-1, 0), part_a, axis, 1)
        c[5] = send(5, (-1, 0), whole, other, 1)
        c[6] = send(6, (-1, 0), whole, other, -1)
        across((-1, 0), (0, 1))
        c[1].wait_recv()
        c[7] = send(7, (1, 0), part_b, axis, -1)
        c[8] = send(8, (1, 0), whole, other, 1)
        c[9] = send(9, (1, 0), whole, other, -1)
        across((1, 0), (0, 1))
        yield
        c[2].wait_recv()
        c[10] = send(10, (0, -1), part_a, other, 1)
        across((0, -1), (0, 1))
        c[3].wait_recv()
        c[11] = send(11, (0, 1), part_b, other, -1)
        across((0, 1), (0, 1))
        yield
        c[4].wait_recv()
        across((2, 0), (0,))
        c[7].wait_recv()
        across((2, 0), (1,))
        c[12] = send(12, (2, 0), whole, other, 1)
        c[13] = send(13, (2, 0), whole, other, -1)
        yield
        c[5].wait_recv()
        c[14] = send(14, (-1, -1), part_a, other, 1)
        across((-1, -1), (0, 1))
        c[6].wait_recv()
        c[15] = send(15, (-1, 1), part_b, other, -1)
        across((-1, 1), (0, 1))
        yield
        c[8].wait_recv()
        c[16] = send(16, (1, -1), part_a, other, 1)
        across((1, -1), (0, 1))
        c[9].wait_recv()
        c[17] = send(17, (1, 1), part_b, other, -1)
        across((1, 1), (0, 1))
        yield
        c[10].wait_recv()
        across((0, 2), (0,))
        c[11].wait_recv()
        across((0, 2), (1,))
        yield
        c[12].wait_recv()
        c[18] = send(18, (2, -1), part_a, other, 1)
        across((2, -1), (0, 1))
        c[13].wait_recv()
        c[19] = send(19, (2, 1), part_b, other, -1)
        across((2, 1), (0, 1))
        yield
        for t, rel, side in ((14, (-1, 2), 0), (15, (-1, 2), 1), (16, (1, 2), 0), (17, (1, 2), 1),
                             (18, (2, 2), 0), (19, (2, 2), 1)):
            c[t].wait_recv()
            across(rel, (side,))
        yield

    def extras():
        mine = pltpu.make_async_copy(tok_ref, all_ref.at[own], local_sem)
        mine.start()
        yield
        gifts = []
        for n, (i, j) in enumerate(offsets):
            gifts.append(go(remote(share_ref.at[here.block("x", i, j)], shares_ref.at[own],
                                   s_send.at[n], s_recv.at[n], here.device(dx=i, dy=j))))
        shares_ref[own] = share_ref[own]
        for n, (src, dst) in enumerate(((wg_ref, wg2_ref), (wu_ref, wu2_ref), (wd_ref, wd2_ref))):
            gifts.append(go(remote(src, dst, w_send.at[n], w_recv.at[n], here.partner())))
            yield
        for _ in range(4):
            yield
        for gift in gifts:
            gift.wait_recv()
        mine.wait()

    fixed = 2 * swap
    flows = []
    for part in range(PARTS):
        flows.append(flow(2 * part, "x", "y", fixed, width - fixed, False))
        flows.append(flow(2 * part + 1, "y", "x", swap_from, swap, True))
    take_turns(flows + [extras()])
    half = swap // 2
    for part in range(PARTS):
        band = pl.ds(part * (rows // PARTS), rows // PARTS)
        for side in (0, 1):
            cols = pl.ds(pl.multiple_of(wanted_from + side * half, unit), half)
            for i, j in offsets:
                ref = all_ref.at[here.block("y", i, j), band, cols]
                slot = i * SIDE + j
                remote(ref, ref, z_send.at[part, side, slot], z_recv.at[part, side, slot],
                       here.device(dz=z_steps[side])).wait_recv()
    for copy in started:
        copy.wait_send()


def gather_all(tokens, share, w_gate, w_up, w_down):
    rows, width = tokens.shape
    vmem, hbm = pl.BlockSpec(memory_space=pltpu.VMEM), pl.BlockSpec(memory_space=pl.ANY)
    dma = pltpu.SemaphoreType.DMA
    like = lambda a: jax.ShapeDtypeStruct(a.shape, a.dtype)
    return pl.pallas_call(
        gather_kernel,
        out_shape=[
            jax.ShapeDtypeStruct((CHIPS, rows, width), BF16),
            like(share), like(w_gate), like(w_up), like(w_down),
        ],
        in_specs=[vmem, vmem, hbm, hbm, hbm],
        out_specs=[hbm, vmem, hbm, hbm, hbm],
        scratch_shapes=[
            dma((2 * PARTS, 20)), dma((2 * PARTS, 20)),
            dma((PARTS, 2, CHIPS)), dma((PARTS, 2, CHIPS)),
            dma((CHIPS - 1,)), dma((CHIPS - 1,)), dma((3,)), dma((3,)), dma(()),
        ],
        compiler_params=pltpu.CompilerParams(
            collective_id=0, has_side_effects=True, vmem_limit_bytes=60 * 2**20
        ),
    )(tokens, share, w_gate, w_up, w_down)


def experts_kernel(
    steps, t_ref, ga_ref, ua_ref, gb_ref, ub_ref, da_ref, db_ref, share_ref, out_ref,
    sums, hidden,
):
    step = pl.program_id(0)
    ff = ga_ref.shape[1]

    @pl.when(step < steps)
    def _():
        w = jnp.concatenate([ga_ref[...], ua_ref[...], gb_ref[...], ub_ref[...]], axis=1)
        more = jnp.dot(t_ref[...], w, preferred_element_type=F32)

        @pl.when(step == 0)
        def _():
            sums[...] = more

        @pl.when(step > 0)
        def _():
            sums[...] += more

    @pl.when(step == steps - 1)
    def _():
        for n in range(2):
            gate = sums[:, 2 * n * ff : (2 * n + 1) * ff]
            up = sums[:, (2 * n + 1) * ff : (2 * n + 2) * ff]
            value = gate / (1.0 + jnp.exp(-gate)) * up
            hidden[:, n * ff : (n + 1) * ff] = (value * share_ref[:, n : n + 1]).astype(BF16)

    @pl.when(step >= steps)
    def _():
        w = jnp.concatenate([da_ref[...], db_ref[...]], axis=0)
        out_ref[...] = jnp.dot(hidden[...], w, preferred_element_type=F32).astype(BF16)


def experts(rows_all, own, other, share):
    rows, width = rows_all.shape
    ff = own[0].shape[1]
    steps = max(1, width // 1792)
    cols = width // steps
    first = lambda i: jnp.minimum(i, steps - 1)
    second = lambda i: jnp.maximum(i - steps, 0)
    up_spec = pl.BlockSpec((cols, ff), lambda i: (first(i), 0))
    down_spec = pl.BlockSpec((ff, cols), lambda i: (0, second(i)))
    return pl.pallas_call(
        functools.partial(experts_kernel, steps),
        grid=(2 * steps,),
        out_shape=jax.ShapeDtypeStruct((rows, width), BF16),
        in_specs=[
            pl.BlockSpec((rows, cols), lambda i: (0, first(i))),
            up_spec, up_spec, up_spec, up_spec, down_spec, down_spec,
            pl.BlockSpec((rows, 2), lambda i: (0, 0)),
        ],
        out_specs=pl.BlockSpec((rows, cols), lambda i: (0, second(i))),
        scratch_shapes=[pltpu.VMEM((rows, 4 * ff), F32), pltpu.VMEM((rows, 2 * ff), BF16)],
        compiler_params=pltpu.CompilerParams(
            dimension_semantics=("arbitrary",), vmem_limit_bytes=58 * 2**20
        ),
        cost_estimate=pl.CostEstimate(
            flops=12 * rows * width * ff,
            bytes_accessed=4 * rows * width + 12 * width * ff,
            transcendentals=2 * rows * ff,
        ),
    )(rows_all, own[0], own[1], other[0], other[1], own[2], other[2], share)


def scatter_kernel(
    layout, part_ref, out_ref, held, swap_in, total, z_in, load_sem, send1, recv1, send2, recv2,
    swap_send, swap_recv, z_send, z_recv, *landing,
):
    here = Place()
    width = held.shape[2]
    group = out_ref.shape[1]
    unit = width // UNITS
    own = here.block("x", 0, 0)
    z_offsets = range(1, here.n_dp)
    greet([here.device(dx=1), here.device(dx=-1), here.device(dy=1), here.device(dy=-1)]
          + [here.device(dz=j) for j in z_offsets])
    started = []
    order = (2, 1, -1, 0)
    steps = (1, -1)
    parity = lax.rem(here.z, 2)
    given_from, kept_from = parity * (width // 4), (1 - parity) * (width // 4)
    given_half = width // 8

    def go(copy):
        copy.start()
        started.append(copy)
        return copy

    def columns(start, span):
        return pl.ds(pl.multiple_of(start, unit), span)

    def swap(part):
        band = pl.ds(*BANDS[part])
        copies = {}
        for a, first in enumerate(order):
            for k, s in enumerate(order):
                block = here.block("y", first, s)
                for side in (0, 1):
                    cols = columns(given_from + side * given_half, given_half)
                    copies[a, k, side] = go(remote(
                        part_ref.at[block, band, cols], swap_in.at[side, 4 * a + k, band],
                        swap_send.at[part, side, 4 * a + k], swap_recv.at[part, side, 4 * a + k],
                        here.device(dz=steps[side])))
        return copies

    def flow(number, part, axis, other, start, spans, swaps):
        half_in, full_in, half_in2, full_in2 = landing[4 * number : 4 * number + 4]
        band = pl.ds(*BANDS[part])
        whole = columns(start, sum(spans))
        parts = (columns(start, spans[0]), columns(start + spans[0], spans[1]))
        slots = (pl.ds(0, spans[0]), pl.ds(0, spans[1]))
        halves, loads = {}, {}
        for a, first in enumerate(order):
            if a == 0 and swaps is None:
                continue
            for k, s in enumerate(order):
                block = here.block(axis, first, s)
                copy = pltpu.make_async_copy(
                    part_ref.at[block, band, whole], held.at[block, band, whole],
                    load_sem.at[number, a, k])
                copy.start()
                loads[a, k] = copy

        def ready(a, k):
            loads[a, k].wait()
            if swaps is None:
                return
            block = here.block(axis, order[a], order[k])
            for side in (0, 1):
                swaps[a, k, side].wait_recv()
                both = held[block, band, parts[side]].astype(F32)
                both += swap_in[side, 4 * a + k, band].astype(F32)
                held[block, band, parts[side]] = both.astype(BF16)

        for k, s in enumerate(order):
            block = here.block(axis, 2, s)
            source = part_ref
            if swaps is not None:
                ready(0, k)
                source = held
            for side in (0, 1):
                halves[k, side] = go(remote(
                    source.at[block, band, parts[side]], half_in.at[side, k, :, slots[side]],
                    send1.at[number, 0, side, k], recv1.at[number, 0, side, k],
                    here.toward(axis, steps[side])))
        yield
        fulls = {}
        for k, s in enumerate(order):
            for side in (0, 1):
                block = here.block(axis, steps[side], s)
                ready(1 + side, k)
                halves[k, side].wait_recv()
                cols = parts[side]
                summed = held[block, band, cols].astype(F32)
                summed += half_in[side, k, :, slots[side]].astype(F32)
                held[block, band, cols] = summed.astype(BF16)
                fulls[k, side] = go(remote(
                    held.at[block, band, whole], full_in.at[side, k],
                    send1.at[number, 1, side, k], recv1.at[number, 1, side, k],
                    here.toward(axis, steps[side])))
            yield

        def settle(k):
            block = here.block(axis, 0, order[k])
            ready(3, k)
            fulls[k, 0].wait_recv()
            fulls[k, 1].wait_recv()
            summed = held[block, band, whole].astype(F32) + full_in[0, k].astype(F32)
            summed += full_in[1, k].astype(F32)
            held[block, band, whole] = summed.astype(BF16)
            return block

        block = settle(0)
        last = []
        for side in (0, 1):
            last.append(go(remote(
                held.at[block, band, parts[side]], half_in2.at[side, :, slots[side]],
                send2.at[number, 0, side], recv2.at[number, 0, side],
                here.toward(other, steps[side]))))
        yield
        blocks = [settle(1), settle(2)]
        yield
        settle(3)
        yield
        finals = []
        for side in (0, 1):
            block, cols = blocks[side], parts[side]
            last[side].wait_recv()
            summed = held[block, band, cols].astype(F32)
            summed += half_in2[side, :, slots[side]].astype(F32)
            held[block, band, cols] = summed.astype(BF16)
            finals.append(go(remote(
                held.at[block, band, whole], full_in2.at[side],
                send2.at[number, 1, side], recv2.at[number, 1, side],
                here.toward(other, steps[side]))))
        yield
        finals[0].wait_recv()
        finals[1].wait_recv()
        summed = held[own, band, whole].astype(F32) + full_in2[0].astype(F32)
        summed += full_in2[1].astype(F32)
        held[own, band, whole] = summed.astype(BF16)
        yield

    quarter = here.n_dp // 4

    def holds(source, target):
        odd = lax.rem(source, 2)
        wanted = jnp.where(target < quarter, 1, 0)
        return jnp.logical_or(target >= 2 * quarter, odd == wanted)

    def group_of(z):
        return columns(z * group, group)

    def spread(part):
        band = pl.ds(*BANDS[part])
        copies = []
        for j in z_offsets:
            target = lax.rem(here.z + j, here.n_dp)
            copy = remote(
                held.at[own, band, group_of(target)], z_in.at[j - 1, band],
                z_send.at[part, j - 1], z_recv.at[part, j - 1], here.device(dz=j))
            pl.when(holds(here.z, target))(copy.start)
            copies.append((copy, target))
        return copies

    def finish(part, copies):
        band = pl.ds(*BANDS[part])
        mine = held[own, band, group_of(here.z)].astype(F32)
        total[band] = jnp.where(holds(here.z, here.z), mine, 0.0)
        for j, (copy, target) in zip(z_offsets, copies):
            source = lax.rem(here.z - j + here.n_dp, here.n_dp)

            @pl.when(holds(source, here.z))
            def _():
                copy.wait_recv()
                total[band] += z_in[j - 1, band].astype(F32)

            pl.when(holds(here.z, target))(copy.wait_send)
        out_ref[band] = total[band].astype(BF16)

    starts = (5 * width // 8, width // 2, kept_from)
    flows, swaps = {}, {}
    axes = (("x", "y"), ("y", "x"), ("y", "x"))

    def begin(name, part):
        n = "abc".index(name)
        flows[name, part] = flow(3 * part + n, part, *axes[n], starts[n], layout[n],
                                 swaps[part] if n == 2 else None)

    def advance(names, part, count):
        for _ in range(count):
            for name in names:
                next(flows[name, part])

    begin("a", 0)
    begin("b", 0)
    advance("ab", 0, 1)
    swaps[0] = swap(0)
    swaps[1] = swap(1)
    begin("c", 0)
    advance("ab", 0, 2)
    advance("c", 0, 1)
    advance("ab", 0, 2)
    advance("c", 0, 2)
    begin("a", 1)
    begin("b", 1)
    advance("ab", 1, 1)
    advance("c", 0, 2)
    advance("ab", 0, 3)
    advance("ab", 1, 2)
    advance("c", 0, 1)
    begin("c", 1)
    advance("c", 1, 1)
    advance("ab", 1, 2)
    advance("ab", 0, 1)
    advance("c", 0, 2)
    advance("c", 1, 4)
    advance("ab", 0, 1)
    advance("c", 0, 1)
    advance("ab", 1, 3)
    advance("c", 0, 1)
    last = [spread(0)]
    advance("c", 1, 3)
    advance("ab", 1, 1)
    advance("c", 1, 1)
    advance("ab", 1, 1)
    advance("c", 1, 1)
    last.append(spread(1))
    for part in range(2):
        finish(part, last[part])
    for copy in started:
        copy.wait_send()


def scatter_all(parts, n_dp):
    blocks, rows, width = parts.shape
    unit, group = width // UNITS, width // n_dp
    layout = ((11 * unit, 10 * unit), (4 * unit, 3 * unit), (7 * unit, 7 * unit))
    dma, vmem = pltpu.SemaphoreType.DMA, pltpu.VMEM
    landing = []
    for part in range(2):
        for first, second in layout:
            band = BANDS[part][1]
            landing += [
                vmem((2, SIDE, band, first), BF16),
                vmem((2, SIDE, band, first + second), BF16),
                vmem((2, band, first), BF16),
                vmem((2, band, first + second), BF16),
            ]
    return pl.pallas_call(
        functools.partial(scatter_kernel, layout),
        out_shape=jax.ShapeDtypeStruct((rows, group), BF16),
        in_specs=[pl.BlockSpec(memory_space=pl.ANY)],
        out_specs=pl.BlockSpec(memory_space=pltpu.VMEM),
        scratch_shapes=[
            vmem((blocks, rows, width), BF16),
            vmem((2, blocks, rows, width // 8), BF16),
            vmem((rows, group), F32),
            vmem((n_dp - 1, rows, group), BF16),
            dma((6, SIDE, SIDE)),
            dma((6, 2, 2, SIDE)), dma((6, 2, 2, SIDE)),
            dma((6, 2, 2)), dma((6, 2, 2)),
            dma((2, 2, blocks)), dma((2, 2, blocks)),
            dma((2, n_dp - 1)), dma((2, n_dp - 1)),
            *landing,
        ],
        compiler_params=pltpu.CompilerParams(
            collective_id=1, has_side_effects=True, vmem_limit_bytes=60 * 2**20
        ),
    )(parts)


def shards(tokens, routes, route_weight, w_gate, w_up, w_down, prev_inputs):
    tok_dev, top = routes.shape
    width = tokens.shape[1]
    n_expert = lax.axis_size("expert")
    n_dp = lax.axis_size("dp")
    col_width = width // n_dp
    counts = route_weight.astype(F32)
    shares = 2.5 * counts / jnp.sum(counts, axis=1, keepdims=True)
    named = jnp.arange(n_expert, dtype=jnp.int32)[:, None, None] == routes[None]
    by_expert = jnp.sum(jnp.where(named, shares[None], 0.0), axis=2)
    by_chip = jnp.broadcast_to(by_expert.reshape(CHIPS, 1, 2 * tok_dev), (CHIPS, 8, 2 * tok_dev))
    whole, arrived, *other = gather_all(tokens, by_chip, w_gate[0], w_up[0], w_down[0])

    history = prev_inputs.reshape(prev_inputs.shape[2], width)
    head = min(HESS_COLS, col_width)
    pieces = jnp.moveaxis(history.reshape(-1, n_dp, col_width), 1, 0)
    heads = jnp.broadcast_to(history[None, :, :head], (n_dp, history.shape[0], head))
    pieces = jnp.concatenate([pieces, heads], axis=2)
    pieces, whole = lax.optimization_barrier((pieces, whole))
    moved = lax.all_to_all(pieces, "dp", split_axis=0, concat_axis=0, tiled=True)

    pairs = arrived[:, 0, :].reshape(CHIPS, 2, tok_dev)
    core = lax.rem(lax.axis_index("expert"), 2)
    pairs = jnp.where(core == 0, pairs, pairs[:, ::-1])
    share = jnp.moveaxis(pairs, 1, 2).reshape(CHIPS * tok_dev, 2)
    out = experts(whole.reshape(CHIPS * tok_dev, width), (w_gate[0], w_up[0], w_down[0]), other, share)
    out, moved = lax.optimization_barrier((out, moved))
    mixed = scatter_all(out.reshape(CHIPS, tok_dev, width), n_dp)

    stacked = moved.reshape(-1, col_width + head)
    hessian = jnp.einsum(
        "rd,rh->dh", stacked[:, :col_width], stacked[:, col_width:], preferred_element_type=F32
    )
    hessian = (hessian * (2.0 / stacked.shape[0]))[:, None, :]
    return (mixed, hessian)


def solution(mesh):
    placed = (
        P("expert", None),
        P("expert", None),
        P("expert", None),
        P("expert", None, "dp"),
        P("expert", None, "dp"),
        P("expert", "dp", None),
        P("dp", "expert", None, None),
    )
    return jax.shard_map(
        shards,
        mesh=mesh,
        in_specs=placed,
        out_specs=(P("expert", "dp"), P("dp", "expert", None)),
        check_vma=False,
    )
```

```python
import functools

import jax
import jax.numpy as jnp
from jax import lax
from jax.experimental import pallas as pl
from jax.experimental.pallas import tpu as pltpu
from jax.sharding import PartitionSpec as P

HESS_COLS = 128
SIDE = 4
CHIPS = SIDE * SIDE
UNITS = 56
SWAP_UNITS = 18
PARTS = 2
BANDS = ((0, 48), (48, 16))
MESH = pl.DeviceIdType.MESH
BF16 = jnp.bfloat16
F32 = jnp.float32


class Place:
    def __init__(self):
        self.n_dp = lax.axis_size("dp")
        self.z = lax.axis_index("dp")
        e = lax.axis_index("expert")
        self.core = lax.rem(e, 2)
        chip = e // 2
        self.y = lax.rem(chip, SIDE)
        self.x = chip // SIDE

    def block(self, axis, first, second):
        dx, dy = (first, second) if axis == "x" else (second, first)
        return lax.rem(self.x + dx + SIDE, SIDE) * SIDE + lax.rem(self.y + dy + SIDE, SIDE)

    def device(self, dx=0, dy=0, dz=0):
        chip = self.block("x", dx, dy)
        return (lax.rem(self.z + dz + self.n_dp, self.n_dp), chip * 2 + self.core)

    def toward(self, axis, step):
        return self.device(dx=step) if axis == "x" else self.device(dy=step)

    def partner(self):
        chip = self.block("x", 0, 0)
        return (self.z, chip * 2 + 1 - self.core)


def greet(devices):
    barrier = pltpu.get_barrier_semaphore()
    for device in devices:
        pl.semaphore_signal(barrier, inc=1, device_id=device, device_id_type=MESH)
    pl.semaphore_wait(barrier, len(devices))


def remote(src, dst, send_sem, recv_sem, device):
    return pltpu.make_async_remote_copy(
        src_ref=src,
        dst_ref=dst,
        send_sem=send_sem,
        recv_sem=recv_sem,
        device_id=device,
        device_id_type=MESH,
    )


def take_turns(flows):
    flows = list(flows)
    while flows:
        left = []
        for flow in flows:
            try:
                next(flow)
                left.append(flow)
            except StopIteration:
                pass
        flows = left


def gather_kernel(
    tok_ref, share_ref, wg_ref, wu_ref, wd_ref,
    all_ref, shares_ref, wg2_ref, wu2_ref, wd2_ref,
    held, flow_send, flow_recv, z_send, z_recv, s_send, s_recv, w_send, w_recv, flush_sem,
):
    here = Place()
    rows, width = tok_ref.shape
    unit = width // UNITS
    offsets = [(i, j) for i in range(SIDE) for j in range(SIDE) if (i, j) != (0, 0)]
    z_steps = (1, -1)
    greet([here.device(dx=i, dy=j) for i, j in offsets]
          + [here.device(dz=s) for s in z_steps] + [here.partner()])
    own = here.block("x", 0, 0)
    started = []

    def go(copy):
        copy.start()
        started.append(copy)
        return copy

    parity = lax.rem(here.z, 2)
    swap = SWAP_UNITS * unit
    swap_from = pl.multiple_of((1 - parity) * swap, unit)
    wanted_from = pl.multiple_of(parity * swap, unit)

    def flow(number, axis, other, start, span, swapped):
        half = span // 2
        band = pl.ds((number // 2) * (rows // PARTS), rows // PARTS)
        whole = pl.ds(start, span)
        part_a, part_b = pl.ds(start, half), pl.ds(pl.multiple_of(start + half, unit), half)

        def send(t, rel, cols, along, step, local=False):
            block = here.block(axis, *rel)
            src = tok_ref.at[band, cols] if local else held.at[block, band, cols]
            return go(remote(src, held.at[block, band, cols], flow_send.at[number, t],
                             flow_recv.at[number, t], here.toward(along, step)))

        def across(rel, which):
            if not swapped:
                return
            block = here.block(axis, *rel)
            slot = (rel[0] % SIDE) * SIDE + rel[1] % SIDE
            for side in which:
                cols = (part_a, part_b)[side]
                ref = held.at[block, band, cols]
                part = number // 2
                go(remote(ref, ref, z_send.at[part, side, slot], z_recv.at[part, side, slot],
                          here.device(dz=z_steps[side])))

        c = {}
        c[0] = send(0, (0, 0), whole, axis, 1, True)
        c[1] = send(1, (0, 0), whole, axis, -1, True)
        yield
        c[2] = send(2, (0, 0), whole, other, 1, True)
        c[3] = send(3, (0, 0), whole, other, -1, True)
        yield
        c[0].wait_recv()
        c[4] = send(4, (-1, 0), part_a, axis, 1)
        c[5] = send(5, (-1, 0), whole, other, 1)
        c[6] = send(6, (-1, 0), whole, other, -1)
        across((-1, 0), (0, 1))
        c[1].wait_recv()
        c[7] = send(7, (1, 0), part_b, axis, -1)
        c[8] = send(8, (1, 0), whole, other, 1)
        c[9] = send(9, (1, 0), whole, other, -1)
        across((1, 0), (0, 1))
        yield
        c[2].wait_recv()
        c[10] = send(10, (0, -1), part_a, other, 1)
        across((0, -1), (0, 1))
        c[3].wait_recv()
        c[11] = send(11, (0, 1), part_b, other, -1)
        across((0, 1), (0, 1))
        yield
        c[4].wait_recv()
        across((2, 0), (0,))
        c[7].wait_recv()
        across((2, 0), (1,))
        c[12] = send(12, (2, 0), whole, other, 1)
        c[13] = send(13, (2, 0), whole, other, -1)
        yield
        c[5].wait_recv()
        c[14] = send(14, (-1, -1), part_a, other, 1)
        across((-1, -1), (0, 1))
        c[6].wait_recv()
        c[15] = send(15, (-1, 1), part_b, other, -1)
        across((-1, 1), (0, 1))
        yield
        c[8].wait_recv()
        c[16] = send(16, (1, -1), part_a, other, 1)
        across((1, -1), (0, 1))
        c[9].wait_recv()
        c[17] = send(17, (1, 1), part_b, other, -1)
        across((1, 1), (0, 1))
        yield
        c[10].wait_recv()
        across((0, 2), (0,))
        c[11].wait_recv()
        across((0, 2), (1,))
        yield
        c[12].wait_recv()
        c[18] = send(18, (2, -1), part_a, other, 1)
        across((2, -1), (0, 1))
        c[13].wait_recv()
        c[19] = send(19, (2, 1), part_b, other, -1)
        across((2, 1), (0, 1))
        yield
        for t, rel, side in ((14, (-1, 2), 0), (15, (-1, 2), 1), (16, (1, 2), 0), (17, (1, 2), 1),
                             (18, (2, 2), 0), (19, (2, 2), 1)):
            c[t].wait_recv()
            across(rel, (side,))
        yield

    def extras():
        yield
        held[own] = tok_ref[...]
        gifts = []
        for n, (i, j) in enumerate(offsets):
            gifts.append(go(remote(share_ref.at[here.block("x", i, j)], shares_ref.at[own],
                                   s_send.at[n], s_recv.at[n], here.device(dx=i, dy=j))))
        shares_ref[own] = share_ref[own]
        for n, (src, dst) in enumerate(((wg_ref, wg2_ref), (wu_ref, wu2_ref), (wd_ref, wd2_ref))):
            gifts.append(go(remote(src, dst, w_send.at[n], w_recv.at[n], here.partner())))
            yield
        for _ in range(4):
            yield
        for gift in gifts:
            gift.wait_recv()

    fixed = 2 * swap
    flows = []
    for part in range(PARTS):
        flows.append(flow(2 * part, "x", "y", fixed, width - fixed, False))
        flows.append(flow(2 * part + 1, "y", "x", swap_from, swap, True))
    take_turns(flows + [extras()])
    flushes = []

    def flush(start, span):
        cols = pl.ds(start, span)
        copy = pltpu.make_async_copy(
            held.at[:, :, cols], all_ref.at[:, :, cols], flush_sem.at[len(flushes)])
        copy.start()
        flushes.append(copy)

    flush(fixed, width - fixed)
    flush(swap_from, swap)
    half = swap // 2
    for part in range(PARTS):
        band = pl.ds(part * (rows // PARTS), rows // PARTS)
        for side in (0, 1):
            cols = pl.ds(pl.multiple_of(wanted_from + side * half, unit), half)
            for i, j in offsets:
                ref = held.at[here.block("y", i, j), band, cols]
                slot = i * SIDE + j
                remote(ref, ref, z_send.at[part, side, slot], z_recv.at[part, side, slot],
                       here.device(dz=z_steps[side])).wait_recv()
    flush(wanted_from, swap)
    for copy in started:
        copy.wait_send()
    for copy in flushes:
        copy.wait()


def gather_all(tokens, share, w_gate, w_up, w_down):
    rows, width = tokens.shape
    vmem, hbm = pl.BlockSpec(memory_space=pltpu.VMEM), pl.BlockSpec(memory_space=pl.ANY)
    dma = pltpu.SemaphoreType.DMA
    like = lambda a: jax.ShapeDtypeStruct(a.shape, a.dtype)
    return pl.pallas_call(
        gather_kernel,
        out_shape=[
            jax.ShapeDtypeStruct((CHIPS, rows, width), BF16),
            like(share), like(w_gate), like(w_up), like(w_down),
        ],
        in_specs=[vmem, vmem, hbm, hbm, hbm],
        out_specs=[hbm, vmem, hbm, hbm, hbm],
        scratch_shapes=[
            pltpu.VMEM((CHIPS, rows, width), BF16),
            dma((2 * PARTS, 20)), dma((2 * PARTS, 20)),
            dma((PARTS, 2, CHIPS)), dma((PARTS, 2, CHIPS)),
            dma((CHIPS - 1,)), dma((CHIPS - 1,)), dma((3,)), dma((3,)), dma((3,)),
        ],
        compiler_params=pltpu.CompilerParams(
            collective_id=0, has_side_effects=True, vmem_limit_bytes=60 * 2**20
        ),
    )(tokens, share, w_gate, w_up, w_down)


def experts_kernel(
    steps, t_ref, ga_ref, ua_ref, gb_ref, ub_ref, da_ref, db_ref, share_ref, out_ref,
    sums, hidden,
):
    step = pl.program_id(0)
    ff = ga_ref.shape[1]

    @pl.when(step < steps)
    def _():
        w = jnp.concatenate([ga_ref[...], ua_ref[...], gb_ref[...], ub_ref[...]], axis=1)
        more = jnp.dot(t_ref[...], w, preferred_element_type=F32)

        @pl.when(step == 0)
        def _():
            sums[...] = more

        @pl.when(step > 0)
        def _():
            sums[...] += more

    @pl.when(step == steps - 1)
    def _():
        for n in range(2):
            gate = sums[:, 2 * n * ff : (2 * n + 1) * ff]
            up = sums[:, (2 * n + 1) * ff : (2 * n + 2) * ff]
            value = gate / (1.0 + jnp.exp(-gate)) * up
            hidden[:, n * ff : (n + 1) * ff] = (value * share_ref[:, n : n + 1]).astype(BF16)

    @pl.when(step >= steps)
    def _():
        w = jnp.concatenate([da_ref[...], db_ref[...]], axis=0)
        out_ref[...] = jnp.dot(hidden[...], w, preferred_element_type=F32).astype(BF16)


def experts(rows_all, own, other, share):
    rows, width = rows_all.shape
    ff = own[0].shape[1]
    steps = max(1, width // 1792)
    cols = width // steps
    first = lambda i: jnp.minimum(i, steps - 1)
    second = lambda i: jnp.maximum(i - steps, 0)
    up_spec = pl.BlockSpec((cols, ff), lambda i: (first(i), 0))
    down_spec = pl.BlockSpec((ff, cols), lambda i: (0, second(i)))
    return pl.pallas_call(
        functools.partial(experts_kernel, steps),
        grid=(2 * steps,),
        out_shape=jax.ShapeDtypeStruct((rows, width), BF16),
        in_specs=[
            pl.BlockSpec((rows, cols), lambda i: (0, first(i))),
            up_spec, up_spec, up_spec, up_spec, down_spec, down_spec,
            pl.BlockSpec((rows, 2), lambda i: (0, 0)),
        ],
        out_specs=pl.BlockSpec((rows, cols), lambda i: (0, second(i))),
        scratch_shapes=[pltpu.VMEM((rows, 4 * ff), F32), pltpu.VMEM((rows, 2 * ff), BF16)],
        compiler_params=pltpu.CompilerParams(
            dimension_semantics=("arbitrary",), vmem_limit_bytes=58 * 2**20
        ),
        cost_estimate=pl.CostEstimate(
            flops=12 * rows * width * ff,
            bytes_accessed=4 * rows * width + 12 * width * ff,
            transcendentals=2 * rows * ff,
        ),
    )(rows_all, own[0], own[1], other[0], other[1], own[2], other[2], share)


def scatter_kernel(
    layout, part_ref, out_ref, held, swap_in, total, z_in, load_sem, send1, recv1, send2, recv2,
    swap_send, swap_recv, z_send, z_recv, *landing,
):
    here = Place()
    width = held.shape[2]
    group = out_ref.shape[1]
    unit = width // UNITS
    own = here.block("x", 0, 0)
    z_offsets = range(1, here.n_dp)
    greet([here.device(dx=1), here.device(dx=-1), here.device(dy=1), here.device(dy=-1)]
          + [here.device(dz=j) for j in z_offsets])
    started = []
    order = (2, 1, -1, 0)
    steps = (1, -1)
    parity = lax.rem(here.z, 2)
    given_from, kept_from = parity * (width // 4), (1 - parity) * (width // 4)
    given_half = width // 8

    def go(copy):
        copy.start()
        started.append(copy)
        return copy

    def columns(start, span):
        return pl.ds(pl.multiple_of(start, unit), span)

    def swap(part):
        band = pl.ds(*BANDS[part])
        copies = {}
        for a, first in enumerate(order):
            line = lax.rem(here.y + first + SIDE, SIDE)
            for side in (0, 1):
                cols = columns(given_from + side * given_half, given_half)
                copies[a, side] = go(remote(
                    part_ref.at[:, line, band, cols], swap_in.at[side, a, :, band],
                    swap_send.at[part, side, a], swap_recv.at[part, side, a],
                    here.device(dz=steps[side])))
        return copies

    def flow(number, part, axis, other, start, spans, swaps):
        half_in, full_in, half_in2, full_in2 = landing[4 * number : 4 * number + 4]
        band = pl.ds(*BANDS[part])
        whole = columns(start, sum(spans))
        parts = (columns(start, spans[0]), columns(start + spans[0], spans[1]))
        slots = (pl.ds(0, spans[0]), pl.ds(0, spans[1]))
        halves, loads = {}, {}
        for a, first in enumerate(order):
            if a == 0 and swaps is None:
                continue
            for k, s in enumerate(order):
                block = here.block(axis, first, s)
                copy = pltpu.make_async_copy(
                    part_ref.at[block // SIDE, lax.rem(block, SIDE), band, whole],
                    held.at[block, band, whole], load_sem.at[number, a, k])
                copy.start()
                loads[a, k] = copy

        def ready(a, k):
            loads[a, k].wait()
            if swaps is None:
                return
            block = here.block(axis, order[a], order[k])
            place = lax.rem(here.x + order[k] + SIDE, SIDE)
            for side in (0, 1):
                if k == 0:
                    swaps[a, side].wait_recv()
                both = held[block, band, parts[side]].astype(F32)
                both += swap_in[side, a, place, band].astype(F32)
                held[block, band, parts[side]] = both.astype(BF16)

        for k, s in enumerate(order):
            block = here.block(axis, 2, s)
            if swaps is not None:
                ready(0, k)
            for side in (0, 1):
                source = held.at[block, band, parts[side]]
                if swaps is None:
                    source = part_ref.at[
                        block // SIDE, lax.rem(block, SIDE), band, parts[side]]
                halves[k, side] = go(remote(
                    source, half_in.at[side, k, :, slots[side]],
                    send1.at[number, 0, side, k], recv1.at[number, 0, side, k],
                    here.toward(axis, steps[side])))
        yield
        fulls = {}
        for k, s in enumerate(order):
            for side in (0, 1):
                block = here.block(axis, steps[side], s)
                ready(1 + side, k)
                halves[k, side].wait_recv()
                cols = parts[side]
                summed = held[block, band, cols].astype(F32)
                summed += half_in[side, k, :, slots[side]].astype(F32)
                held[block, band, cols] = summed.astype(BF16)
                fulls[k, side] = go(remote(
                    held.at[block, band, whole], full_in.at[side, k],
                    send1.at[number, 1, side, k], recv1.at[number, 1, side, k],
                    here.toward(axis, steps[side])))
            yield

        def settle(k):
            block = here.block(axis, 0, order[k])
            ready(3, k)
            fulls[k, 0].wait_recv()
            fulls[k, 1].wait_recv()
            summed = held[block, band, whole].astype(F32) + full_in[0, k].astype(F32)
            summed += full_in[1, k].astype(F32)
            held[block, band, whole] = summed.astype(BF16)
            return block

        block = settle(0)
        last = []
        for side in (0, 1):
            last.append(go(remote(
                held.at[block, band, parts[side]], half_in2.at[side, :, slots[side]],
                send2.at[number, 0, side], recv2.at[number, 0, side],
                here.toward(other, steps[side]))))
        yield
        blocks = [settle(1), settle(2)]
        yield
        settle(3)
        yield
        finals = []
        for side in (0, 1):
            block, cols = blocks[side], parts[side]
            last[side].wait_recv()
            summed = held[block, band, cols].astype(F32)
            summed += half_in2[side, :, slots[side]].astype(F32)
            held[block, band, cols] = summed.astype(BF16)
            finals.append(go(remote(
                held.at[block, band, whole], full_in2.at[side],
                send2.at[number, 1, side], recv2.at[number, 1, side],
                here.toward(other, steps[side]))))
        yield
        finals[0].wait_recv()
        finals[1].wait_recv()
        summed = held[own, band, whole].astype(F32) + full_in2[0].astype(F32)
        summed += full_in2[1].astype(F32)
        held[own, band, whole] = summed.astype(BF16)
        yield

    quarter = here.n_dp // 4

    def holds(source, target):
        odd = lax.rem(source, 2)
        wanted = jnp.where(target < quarter, 1, 0)
        return jnp.logical_or(target >= 2 * quarter, odd == wanted)

    def group_of(z):
        return columns(z * group, group)

    def spread(part):
        band = pl.ds(*BANDS[part])
        copies = []
        for j in z_offsets:
            target = lax.rem(here.z + j, here.n_dp)
            copy = remote(
                held.at[own, band, group_of(target)], z_in.at[j - 1, band],
                z_send.at[part, j - 1], z_recv.at[part, j - 1], here.device(dz=j))
            pl.when(holds(here.z, target))(copy.start)
            copies.append((copy, target))
        return copies

    def finish(part, copies):
        band = pl.ds(*BANDS[part])
        mine = held[own, band, group_of(here.z)].astype(F32)
        total[band] = jnp.where(holds(here.z, here.z), mine, 0.0)
        for j, (copy, target) in zip(z_offsets, copies):
            source = lax.rem(here.z - j + here.n_dp, here.n_dp)

            @pl.when(holds(source, here.z))
            def _():
                copy.wait_recv()
                total[band] += z_in[j - 1, band].astype(F32)

            pl.when(holds(here.z, target))(copy.wait_send)
        out_ref[band] = total[band].astype(BF16)

    starts = (5 * width // 8, width // 2, kept_from)
    flows, swaps = {}, {}
    axes = (("x", "y"), ("y", "x"), ("y", "x"))

    def begin(name, part):
        n = "abc".index(name)
        flows[name, part] = flow(3 * part + n, part, *axes[n], starts[n], layout[n],
                                 swaps[part] if n == 2 else None)

    def advance(names, part, count):
        for _ in range(count):
            for name in names:
                next(flows[name, part])

    begin("a", 0)
    begin("b", 0)
    advance("ab", 0, 1)
    swaps[0] = swap(0)
    swaps[1] = swap(1)
    begin("c", 0)
    advance("ab", 0, 2)
    advance("c", 0, 1)
    advance("ab", 0, 2)
    advance("c", 0, 2)
    begin("a", 1)
    begin("b", 1)
    advance("ab", 1, 1)
    advance("c", 0, 2)
    advance("ab", 0, 3)
    advance("ab", 1, 2)
    advance("c", 0, 1)
    begin("c", 1)
    advance("c", 1, 1)
    advance("ab", 1, 2)
    advance("ab", 0, 1)
    advance("c", 0, 2)
    advance("c", 1, 4)
    advance("ab", 0, 1)
    advance("c", 0, 1)
    advance("ab", 1, 3)
    advance("c", 0, 1)
    last = [spread(0)]
    advance("c", 1, 3)
    advance("ab", 1, 1)
    advance("c", 1, 1)
    advance("ab", 1, 1)
    advance("c", 1, 1)
    last.append(spread(1))
    for part in range(2):
        finish(part, last[part])
    for copy in started:
        copy.wait_send()


def scatter_all(parts, n_dp):
    blocks, rows, width = parts.shape
    unit, group = width // UNITS, width // n_dp
    layout = ((11 * unit, 10 * unit), (4 * unit, 3 * unit), (7 * unit, 7 * unit))
    dma, vmem = pltpu.SemaphoreType.DMA, pltpu.VMEM
    landing = []
    for part in range(2):
        for first, second in layout:
            band = BANDS[part][1]
            landing += [
                vmem((2, SIDE, band, first), BF16),
                vmem((2, SIDE, band, first + second), BF16),
                vmem((2, band, first), BF16),
                vmem((2, band, first + second), BF16),
            ]
    return pl.pallas_call(
        functools.partial(scatter_kernel, layout),
        out_shape=jax.ShapeDtypeStruct((rows, group), BF16),
        in_specs=[pl.BlockSpec(memory_space=pl.ANY)],
        out_specs=pl.BlockSpec(memory_space=pltpu.VMEM),
        scratch_shapes=[
            vmem((blocks, rows, width), BF16),
            vmem((2, SIDE, SIDE, rows, width // 8), BF16),
            vmem((rows, group), F32),
            vmem((n_dp - 1, rows, group), BF16),
            dma((6, SIDE, SIDE)),
            dma((6, 2, 2, SIDE)), dma((6, 2, 2, SIDE)),
            dma((6, 2, 2)), dma((6, 2, 2)),
            dma((2, 2, SIDE)), dma((2, 2, SIDE)),
            dma((2, n_dp - 1)), dma((2, n_dp - 1)),
            *landing,
        ],
        compiler_params=pltpu.CompilerParams(
            collective_id=1, has_side_effects=True, vmem_limit_bytes=60 * 2**20
        ),
    )(parts.reshape(SIDE, SIDE, rows, width))


def shards(tokens, routes, route_weight, w_gate, w_up, w_down, prev_inputs):
    tok_dev, top = routes.shape
    width = tokens.shape[1]
    n_expert = lax.axis_size("expert")
    n_dp = lax.axis_size("dp")
    col_width = width // n_dp
    counts = route_weight.astype(F32)
    shares = 2.5 * counts / jnp.sum(counts, axis=1, keepdims=True)
    named = jnp.arange(n_expert, dtype=jnp.int32)[:, None, None] == routes[None]
    by_expert = jnp.sum(jnp.where(named, shares[None], 0.0), axis=2)
    by_chip = jnp.broadcast_to(by_expert.reshape(CHIPS, 1, 2 * tok_dev), (CHIPS, 8, 2 * tok_dev))
    whole, arrived, *other = gather_all(tokens, by_chip, w_gate[0], w_up[0], w_down[0])

    history = prev_inputs.reshape(prev_inputs.shape[2], width)
    head = min(HESS_COLS, col_width)
    pieces = jnp.moveaxis(history.reshape(-1, n_dp, col_width), 1, 0)
    heads = jnp.broadcast_to(history[None, :, :head], (n_dp, history.shape[0], head))
    pieces = jnp.concatenate([pieces, heads], axis=2)
    pieces, whole = lax.optimization_barrier((pieces, whole))
    moved = lax.all_to_all(pieces, "dp", split_axis=0, concat_axis=0, tiled=True)

    pairs = arrived[:, 0, :].reshape(CHIPS, 2, tok_dev)
    core = lax.rem(lax.axis_index("expert"), 2)
    pairs = jnp.where(core == 0, pairs, pairs[:, ::-1])
    share = jnp.moveaxis(pairs, 1, 2).reshape(CHIPS * tok_dev, 2)
    out = experts(whole.reshape(CHIPS * tok_dev, width), (w_gate[0], w_up[0], w_down[0]), other, share)
    out, moved = lax.optimization_barrier((out, moved))
    mixed = scatter_all(out.reshape(CHIPS, tok_dev, width), n_dp)

    stacked = moved.reshape(-1, col_width + head)
    hessian = jnp.einsum(
        "rd,rh->dh", stacked[:, :col_width], stacked[:, col_width:], preferred_element_type=F32
    )
    hessian = (hessian * (2.0 / stacked.shape[0]))[:, None, :]
    return (mixed, hessian)


def solution(mesh):
    placed = (
        P("expert", None),
        P("expert", None),
        P("expert", None),
        P("expert", None, "dp"),
        P("expert", None, "dp"),
        P("expert", "dp", None),
        P("dp", "expert", None, None),
    )
    return jax.shard_map(
        shards,
        mesh=mesh,
        in_specs=placed,
        out_specs=(P("expert", "dp"), P("dp", "expert", None)),
        check_vma=False,
    )
```

```python
import functools

import jax
import jax.numpy as jnp
from jax import lax
from jax.experimental import pallas as pl
from jax.experimental.pallas import tpu as pltpu
from jax.sharding import PartitionSpec as P

HESS_COLS = 128
SIDE = 4
CHIPS = SIDE * SIDE
UNITS = 56
SWAP_UNITS = 18
PARTS = 2
BANDS = ((0, 48), (48, 16))
GATHER_ORDER = "1313210121032331010211332223322001203000"
SCATTER_ORDER = "014S1011042414000222210230T11102225330412553435534554545333435"
MESH = pl.DeviceIdType.MESH
BF16 = jnp.bfloat16
F32 = jnp.float32


class Place:
    def __init__(self):
        self.n_dp = lax.axis_size("dp")
        self.z = lax.axis_index("dp")
        e = lax.axis_index("expert")
        self.core = lax.rem(e, 2)
        chip = e // 2
        self.y = lax.rem(chip, SIDE)
        self.x = chip // SIDE

    def block(self, axis, first, second):
        dx, dy = (first, second) if axis == "x" else (second, first)
        return lax.rem(self.x + dx + SIDE, SIDE) * SIDE + lax.rem(self.y + dy + SIDE, SIDE)

    def device(self, dx=0, dy=0, dz=0):
        chip = self.block("x", dx, dy)
        return (lax.rem(self.z + dz + self.n_dp, self.n_dp), chip * 2 + self.core)

    def toward(self, axis, step):
        return self.device(dx=step) if axis == "x" else self.device(dy=step)

    def partner(self):
        chip = self.block("x", 0, 0)
        return (self.z, chip * 2 + 1 - self.core)


def greet(devices):
    barrier = pltpu.get_barrier_semaphore()
    for device in devices:
        pl.semaphore_signal(barrier, inc=1, device_id=device, device_id_type=MESH)
    pl.semaphore_wait(barrier, len(devices))


def remote(src, dst, send_sem, recv_sem, device):
    return pltpu.make_async_remote_copy(
        src_ref=src,
        dst_ref=dst,
        send_sem=send_sem,
        recv_sem=recv_sem,
        device_id=device,
        device_id_type=MESH,
    )


def take_turns(flows):
    flows = list(flows)
    while flows:
        left = []
        for flow in flows:
            try:
                next(flow)
                left.append(flow)
            except StopIteration:
                pass
        flows = left


def gather_kernel(
    tok_ref, share_ref, wg_ref, wu_ref, wd_ref,
    all_ref, shares_ref, wg2_ref, wu2_ref, wd2_ref,
    flow_send, flow_recv, z_send, z_recv, s_send, s_recv, w_send, w_recv, local_sem,
):
    here = Place()
    rows, width = tok_ref.shape
    unit = width // UNITS
    offsets = [(i, j) for i in range(SIDE) for j in range(SIDE) if (i, j) != (0, 0)]
    z_steps = (1, -1)
    greet([here.device(dx=i, dy=j) for i, j in offsets]
          + [here.device(dz=s) for s in z_steps] + [here.partner()])
    own = here.block("x", 0, 0)
    started = []

    def go(copy):
        copy.start()
        started.append(copy)
        return copy

    parity = lax.rem(here.z, 2)
    swap = SWAP_UNITS * unit
    swap_from = pl.multiple_of((1 - parity) * swap, unit)
    wanted_from = pl.multiple_of(parity * swap, unit)

    def flow(number, axis, other, start, span, swapped):
        half = span // 2
        band = pl.ds((number // 2) * (rows // PARTS), rows // PARTS)
        whole = pl.ds(start, span)
        part_a, part_b = pl.ds(start, half), pl.ds(pl.multiple_of(start + half, unit), half)

        def send(t, rel, cols, along, step, local=False):
            block = here.block(axis, *rel)
            src = tok_ref.at[band, cols] if local else all_ref.at[block, band, cols]
            return go(remote(src, all_ref.at[block, band, cols], flow_send.at[number, t],
                             flow_recv.at[number, t], here.toward(along, step)))

        def across(rel, which):
            if not swapped:
                return
            block = here.block(axis, *rel)
            slot = (rel[0] % SIDE) * SIDE + rel[1] % SIDE
            for side in which:
                cols = (part_a, part_b)[side]
                ref = all_ref.at[block, band, cols]
                part = number // 2
                go(remote(ref, ref, z_send.at[part, side, slot], z_recv.at[part, side, slot],
                          here.device(dz=z_steps[side])))

        c = {}
        c[0] = send(0, (0, 0), whole, axis, 1, True)
        c[1] = send(1, (0, 0), whole, axis, -1, True)
        yield
        c[2] = send(2, (0, 0), whole, other, 1, True)
        c[3] = send(3, (0, 0), whole, other, -1, True)
        yield
        c[0].wait_recv()
        c[4] = send(4, (-1, 0), part_a, axis, 1)
        c[5] = send(5, (-1, 0), whole, other, 1)
        c[6] = send(6, (-1, 0), whole, other, -1)
        across((-1, 0), (0, 1))
        c[1].wait_recv()
        c[7] = send(7, (1, 0), part_b, axis, -1)
        c[8] = send(8, (1, 0), whole, other, 1)
        c[9] = send(9, (1, 0), whole, other, -1)
        across((1, 0), (0, 1))
        yield
        c[2].wait_recv()
        c[10] = send(10, (0, -1), part_a, other, 1)
        across((0, -1), (0, 1))
        c[3].wait_recv()
        c[11] = send(11, (0, 1), part_b, other, -1)
        across((0, 1), (0, 1))
        yield
        c[4].wait_recv()
        across((2, 0), (0,))
        c[7].wait_recv()
        across((2, 0), (1,))
        c[12] = send(12, (2, 0), whole, other, 1)
        c[13] = send(13, (2, 0), whole, other, -1)
        yield
        c[5].wait_recv()
        c[14] = send(14, (-1, -1), part_a, other, 1)
        across((-1, -1), (0, 1))
        c[6].wait_recv()
        c[15] = send(15, (-1, 1), part_b, other, -1)
        across((-1, 1), (0, 1))
        yield
        c[8].wait_recv()
        c[16] = send(16, (1, -1), part_a, other, 1)
        across((1, -1), (0, 1))
        c[9].wait_recv()
        c[17] = send(17, (1, 1), part_b, other, -1)
        across((1, 1), (0, 1))
        yield
        c[10].wait_recv()
        across((0, 2), (0,))
        c[11].wait_recv()
        across((0, 2), (1,))
        yield
        c[12].wait_recv()
        c[18] = send(18, (2, -1), part_a, other, 1)
        across((2, -1), (0, 1))
        c[13].wait_recv()
        c[19] = send(19, (2, 1), part_b, other, -1)
        across((2, 1), (0, 1))
        yield
        for t, rel, side in ((14, (-1, 2), 0), (15, (-1, 2), 1), (16, (1, 2), 0), (17, (1, 2), 1),
                             (18, (2, 2), 0), (19, (2, 2), 1)):
            c[t].wait_recv()
            across(rel, (side,))
        yield

    def extras():
        mine = pltpu.make_async_copy(tok_ref, all_ref.at[own], local_sem)
        mine.start()
        yield
        gifts = []
        for n, (i, j) in enumerate(offsets):
            gifts.append(go(remote(share_ref.at[here.block("x", i, j)], shares_ref.at[own],
                                   s_send.at[n], s_recv.at[n], here.device(dx=i, dy=j))))
        shares_ref[own] = share_ref[own]
        for n, (src, dst) in enumerate(((wg_ref, wg2_ref), (wu_ref, wu2_ref), (wd_ref, wd2_ref))):
            gifts.append(go(remote(src, dst, w_send.at[n], w_recv.at[n], here.partner())))
            yield
        for _ in range(4):
            yield
        for gift in gifts:
            gift.wait_recv()
        mine.wait()

    fixed = 2 * swap
    flows = []
    for part in range(PARTS):
        flows.append(flow(2 * part, "x", "y", fixed, width - fixed, False))
        flows.append(flow(2 * part + 1, "y", "x", swap_from, swap, True))
    flows.append(extras())
    for n, turn in enumerate(GATHER_ORDER):
        next(flows[int(turn)])
        if n % 4 == 0 and 0 < n < 36:
            next(flows[-1])
    take_turns(flows[-1:])
    half = swap // 2
    for part in range(PARTS):
        band = pl.ds(part * (rows // PARTS), rows // PARTS)
        for side in (0, 1):
            cols = pl.ds(pl.multiple_of(wanted_from + side * half, unit), half)
            for i, j in offsets:
                ref = all_ref.at[here.block("y", i, j), band, cols]
                slot = i * SIDE + j
                remote(ref, ref, z_send.at[part, side, slot], z_recv.at[part, side, slot],
                       here.device(dz=z_steps[side])).wait_recv()
    for copy in started:
        copy.wait_send()


def gather_all(tokens, share, w_gate, w_up, w_down):
    rows, width = tokens.shape
    vmem, hbm = pl.BlockSpec(memory_space=pltpu.VMEM), pl.BlockSpec(memory_space=pl.ANY)
    dma = pltpu.SemaphoreType.DMA
    like = lambda a: jax.ShapeDtypeStruct(a.shape, a.dtype)
    return pl.pallas_call(
        gather_kernel,
        out_shape=[
            jax.ShapeDtypeStruct((CHIPS, rows, width), BF16),
            like(share), like(w_gate), like(w_up), like(w_down),
        ],
        in_specs=[vmem, vmem, hbm, hbm, hbm],
        out_specs=[hbm, vmem, hbm, hbm, hbm],
        scratch_shapes=[
            dma((2 * PARTS, 20)), dma((2 * PARTS, 20)),
            dma((PARTS, 2, CHIPS)), dma((PARTS, 2, CHIPS)),
            dma((CHIPS - 1,)), dma((CHIPS - 1,)), dma((3,)), dma((3,)), dma(()),
        ],
        compiler_params=pltpu.CompilerParams(
            collective_id=0, has_side_effects=True, vmem_limit_bytes=60 * 2**20
        ),
    )(tokens, share, w_gate, w_up, w_down)


def experts_kernel(
    steps, t_ref, ga_ref, ua_ref, gb_ref, ub_ref, da_ref, db_ref, share_ref, out_ref,
    sums, hidden,
):
    step = pl.program_id(0)
    ff = ga_ref.shape[1]

    @pl.when(step < steps)
    def _():
        w = jnp.concatenate([ga_ref[...], ua_ref[...], gb_ref[...], ub_ref[...]], axis=1)
        more = jnp.dot(t_ref[...], w, preferred_element_type=F32)

        @pl.when(step == 0)
        def _():
            sums[...] = more

        @pl.when(step > 0)
        def _():
            sums[...] += more

    @pl.when(step == steps - 1)
    def _():
        for n in range(2):
            gate = sums[:, 2 * n * ff : (2 * n + 1) * ff]
            up = sums[:, (2 * n + 1) * ff : (2 * n + 2) * ff]
            value = gate / (1.0 + jnp.exp(-gate)) * up
            hidden[:, n * ff : (n + 1) * ff] = (value * share_ref[:, n : n + 1]).astype(BF16)

    @pl.when(step >= steps)
    def _():
        w = jnp.concatenate([da_ref[...], db_ref[...]], axis=0)
        out_ref[...] = jnp.dot(hidden[...], w, preferred_element_type=F32).astype(BF16)


def experts(rows_all, own, other, share):
    rows, width = rows_all.shape
    ff = own[0].shape[1]
    steps = max(1, width // 1792)
    cols = width // steps
    first = lambda i: jnp.minimum(i, steps - 1)
    second = lambda i: jnp.maximum(i - steps, 0)
    up_spec = pl.BlockSpec((cols, ff), lambda i: (first(i), 0))
    down_spec = pl.BlockSpec((ff, cols), lambda i: (0, second(i)))
    return pl.pallas_call(
        functools.partial(experts_kernel, steps),
        grid=(2 * steps,),
        out_shape=jax.ShapeDtypeStruct((rows, width), BF16),
        in_specs=[
            pl.BlockSpec((rows, cols), lambda i: (0, first(i))),
            up_spec, up_spec, up_spec, up_spec, down_spec, down_spec,
            pl.BlockSpec((rows, 2), lambda i: (0, 0)),
        ],
        out_specs=pl.BlockSpec((rows, cols), lambda i: (0, second(i))),
        scratch_shapes=[pltpu.VMEM((rows, 4 * ff), F32), pltpu.VMEM((rows, 2 * ff), BF16)],
        compiler_params=pltpu.CompilerParams(
            dimension_semantics=("arbitrary",), vmem_limit_bytes=58 * 2**20
        ),
        cost_estimate=pl.CostEstimate(
            flops=12 * rows * width * ff,
            bytes_accessed=4 * rows * width + 12 * width * ff,
            transcendentals=2 * rows * ff,
        ),
    )(rows_all, own[0], own[1], other[0], other[1], own[2], other[2], share)


def scatter_kernel(
    layout, part_ref, out_ref, held, swap_in, total, z_in, load_sem, send1, recv1, send2, recv2,
    swap_send, swap_recv, z_send, z_recv, *landing,
):
    here = Place()
    width = held.shape[2]
    group = out_ref.shape[1]
    unit = width // UNITS
    own = here.block("x", 0, 0)
    z_offsets = range(1, here.n_dp)
    greet([here.device(dx=1), here.device(dx=-1), here.device(dy=1), here.device(dy=-1)]
          + [here.device(dz=j) for j in z_offsets])
    started = []
    order = (2, 1, -1, 0)
    steps = (1, -1)
    parity = lax.rem(here.z, 2)
    given_from, kept_from = parity * (width // 4), (1 - parity) * (width // 4)
    given_half = width // 8

    def go(copy):
        copy.start()
        started.append(copy)
        return copy

    def columns(start, span):
        return pl.ds(pl.multiple_of(start, unit), span)

    def swap(part):
        band = pl.ds(*BANDS[part])
        copies = {}
        for a, first in enumerate(order):
            line = lax.rem(here.y + first + SIDE, SIDE)
            for side in (0, 1):
                cols = columns(given_from + side * given_half, given_half)
                copies[a, side] = go(remote(
                    part_ref.at[:, line, band, cols], swap_in.at[side, a, :, band],
                    swap_send.at[part, side, a], swap_recv.at[part, side, a],
                    here.device(dz=steps[side])))
        return copies

    def flow(number, part, axis, other, start, spans, swaps):
        half_in, full_in, half_in2, full_in2 = landing[4 * number : 4 * number + 4]
        band = pl.ds(*BANDS[part])
        whole = columns(start, sum(spans))
        parts = (columns(start, spans[0]), columns(start + spans[0], spans[1]))
        slots = (pl.ds(0, spans[0]), pl.ds(0, spans[1]))
        halves, loads = {}, {}
        for a, first in enumerate(order):
            if a == 0 and swaps is None:
                continue
            for k, s in enumerate(order):
                block = here.block(axis, first, s)
                copy = pltpu.make_async_copy(
                    part_ref.at[block // SIDE, lax.rem(block, SIDE), band, whole],
                    held.at[block, band, whole], load_sem.at[number, a, k])
                copy.start()
                loads[a, k] = copy

        def ready(a, k):
            loads[a, k].wait()
            if swaps is None:
                return
            block = here.block(axis, order[a], order[k])
            place = lax.rem(here.x + order[k] + SIDE, SIDE)
            for side in (0, 1):
                if k == 0:
                    swaps[a, side].wait_recv()
                both = held[block, band, parts[side]].astype(F32)
                both += swap_in[side, a, place, band].astype(F32)
                held[block, band, parts[side]] = both.astype(BF16)

        for k, s in enumerate(order):
            block = here.block(axis, 2, s)
            if swaps is not None:
                ready(0, k)
            for side in (0, 1):
                source = held.at[block, band, parts[side]]
                if swaps is None:
                    source = part_ref.at[
                        block // SIDE, lax.rem(block, SIDE), band, parts[side]]
                halves[k, side] = go(remote(
                    source, half_in.at[side, k, :, slots[side]],
                    send1.at[number, 0, side, k], recv1.at[number, 0, side, k],
                    here.toward(axis, steps[side])))
        yield
        fulls = {}
        for k, s in enumerate(order):
            for side in (0, 1):
                block = here.block(axis, steps[side], s)
                ready(1 + side, k)
                halves[k, side].wait_recv()
                cols = parts[side]
                summed = held[block, band, cols].astype(F32)
                summed += half_in[side, k, :, slots[side]].astype(F32)
                held[block, band, cols] = summed.astype(BF16)
                fulls[k, side] = go(remote(
                    held.at[block, band, whole], full_in.at[side, k],
                    send1.at[number, 1, side, k], recv1.at[number, 1, side, k],
                    here.toward(axis, steps[side])))
            yield

        def settle(k):
            block = here.block(axis, 0, order[k])
            ready(3, k)
            fulls[k, 0].wait_recv()
            fulls[k, 1].wait_recv()
            summed = held[block, band, whole].astype(F32) + full_in[0, k].astype(F32)
            summed += full_in[1, k].astype(F32)
            held[block, band, whole] = summed.astype(BF16)
            return block

        block = settle(0)
        last = []
        for side in (0, 1):
            last.append(go(remote(
                held.at[block, band, parts[side]], half_in2.at[side, :, slots[side]],
                send2.at[number, 0, side], recv2.at[number, 0, side],
                here.toward(other, steps[side]))))
        yield
        blocks = [settle(1), settle(2)]
        yield
        settle(3)
        yield
        finals = []
        for side in (0, 1):
            block, cols = blocks[side], parts[side]
            last[side].wait_recv()
            summed = held[block, band, cols].astype(F32)
            summed += half_in2[side, :, slots[side]].astype(F32)
            held[block, band, cols] = summed.astype(BF16)
            finals.append(go(remote(
                held.at[block, band, whole], full_in2.at[side],
                send2.at[number, 1, side], recv2.at[number, 1, side],
                here.toward(other, steps[side]))))
        yield
        finals[0].wait_recv()
        finals[1].wait_recv()
        summed = held[own, band, whole].astype(F32) + full_in2[0].astype(F32)
        summed += full_in2[1].astype(F32)
        held[own, band, whole] = summed.astype(BF16)
        yield

    quarter = here.n_dp // 4

    def holds(source, target):
        odd = lax.rem(source, 2)
        wanted = jnp.where(target < quarter, 1, 0)
        return jnp.logical_or(target >= 2 * quarter, odd == wanted)

    def group_of(z):
        return columns(z * group, group)

    def spread(part):
        band = pl.ds(*BANDS[part])
        copies = []
        for j in z_offsets:
            target = lax.rem(here.z + j, here.n_dp)
            copy = remote(
                held.at[own, band, group_of(target)], z_in.at[j - 1, band],
                z_send.at[part, j - 1], z_recv.at[part, j - 1], here.device(dz=j))
            pl.when(holds(here.z, target))(copy.start)
            copies.append((copy, target))
        return copies

    def finish(part, copies):
        band = pl.ds(*BANDS[part])
        mine = held[own, band, group_of(here.z)].astype(F32)
        total[band] = jnp.where(holds(here.z, here.z), mine, 0.0)
        for j, (copy, target) in zip(z_offsets, copies):
            source = lax.rem(here.z - j + here.n_dp, here.n_dp)

            @pl.when(holds(source, here.z))
            def _():
                copy.wait_recv()
                total[band] += z_in[j - 1, band].astype(F32)

            pl.when(holds(here.z, target))(copy.wait_send)
        out_ref[band] = total[band].astype(BF16)

    starts = (5 * width // 8, width // 2, kept_from)
    flows, swaps = {}, {}
    axes = (("x", "y"), ("y", "x"), ("y", "x"))

    def begin(name, part):
        n = "abc".index(name)
        flows[name, part] = flow(3 * part + n, part, *axes[n], starts[n], layout[n],
                                 swaps[part] if n == 2 else None)

    turns, last = {}, {}
    for turn in SCATTER_ORDER:
        if turn in "ST":
            part = "ST".index(turn)
            swaps[part] = swap(part)
            continue
        part, name = int(turn) // 3, "abc"[int(turn) % 3]
        if (name, part) not in flows:
            begin(name, part)
        next(flows[name, part])
        turns[part] = turns.get(part, 0) + 1
        if turns[part] == 30:
            last[part] = spread(part)
    for part in range(2):
        finish(part, last[part])
    for copy in started:
        copy.wait_send()


def scatter_all(parts, n_dp):
    blocks, rows, width = parts.shape
    unit, group = width // UNITS, width // n_dp
    layout = ((11 * unit, 10 * unit), (4 * unit, 3 * unit), (7 * unit, 7 * unit))
    dma, vmem = pltpu.SemaphoreType.DMA, pltpu.VMEM
    landing = []
    for part in range(2):
        for first, second in layout:
            band = BANDS[part][1]
            landing += [
                vmem((2, SIDE, band, first), BF16),
                vmem((2, SIDE, band, first + second), BF16),
                vmem((2, band, first), BF16),
                vmem((2, band, first + second), BF16),
            ]
    return pl.pallas_call(
        functools.partial(scatter_kernel, layout),
        out_shape=jax.ShapeDtypeStruct((rows, group), BF16),
        in_specs=[pl.BlockSpec(memory_space=pl.ANY)],
        out_specs=pl.BlockSpec(memory_space=pltpu.VMEM),
        scratch_shapes=[
            vmem((blocks, rows, width), BF16),
            vmem((2, SIDE, SIDE, rows, width // 8), BF16),
            vmem((rows, group), F32),
            vmem((n_dp - 1, rows, group), BF16),
            dma((6, SIDE, SIDE)),
            dma((6, 2, 2, SIDE)), dma((6, 2, 2, SIDE)),
            dma((6, 2, 2)), dma((6, 2, 2)),
            dma((2, 2, SIDE)), dma((2, 2, SIDE)),
            dma((2, n_dp - 1)), dma((2, n_dp - 1)),
            *landing,
        ],
        compiler_params=pltpu.CompilerParams(
            collective_id=1, has_side_effects=True, vmem_limit_bytes=60 * 2**20
        ),
    )(parts.reshape(SIDE, SIDE, rows, width))


def shards(tokens, routes, route_weight, w_gate, w_up, w_down, prev_inputs):
    tok_dev, top = routes.shape
    width = tokens.shape[1]
    n_expert = lax.axis_size("expert")
    n_dp = lax.axis_size("dp")
    col_width = width // n_dp
    counts = route_weight.astype(F32)
    shares = 2.5 * counts / jnp.sum(counts, axis=1, keepdims=True)
    named = jnp.arange(n_expert, dtype=jnp.int32)[:, None, None] == routes[None]
    by_expert = jnp.sum(jnp.where(named, shares[None], 0.0), axis=2)
    by_chip = jnp.broadcast_to(by_expert.reshape(CHIPS, 1, 2 * tok_dev), (CHIPS, 8, 2 * tok_dev))
    whole, arrived, *other = gather_all(tokens, by_chip, w_gate[0], w_up[0], w_down[0])

    history = prev_inputs.reshape(prev_inputs.shape[2], width)
    head = min(HESS_COLS, col_width)
    pieces = jnp.moveaxis(history.reshape(-1, n_dp, col_width), 1, 0)
    heads = jnp.broadcast_to(history[None, :, :head], (n_dp, history.shape[0], head))
    pieces = jnp.concatenate([pieces, heads], axis=2)
    pieces, whole = lax.optimization_barrier((pieces, whole))
    moved = lax.all_to_all(pieces, "dp", split_axis=0, concat_axis=0, tiled=True)

    pairs = arrived[:, 0, :].reshape(CHIPS, 2, tok_dev)
    core = lax.rem(lax.axis_index("expert"), 2)
    pairs = jnp.where(core == 0, pairs, pairs[:, ::-1])
    share = jnp.moveaxis(pairs, 1, 2).reshape(CHIPS * tok_dev, 2)
    out = experts(whole.reshape(CHIPS * tok_dev, width), (w_gate[0], w_up[0], w_down[0]), other, share)
    out, moved = lax.optimization_barrier((out, moved))
    mixed = scatter_all(out.reshape(CHIPS, tok_dev, width), n_dp)

    stacked = moved.reshape(-1, col_width + head)
    hessian = jnp.einsum(
        "rd,rh->dh", stacked[:, :col_width], stacked[:, col_width:], preferred_element_type=F32
    )
    hessian = (hessian * (2.0 / stacked.shape[0]))[:, None, :]
    return (mixed, hessian)


def solution(mesh):
    placed = (
        P("expert", None),
        P("expert", None),
        P("expert", None),
        P("expert", None, "dp"),
        P("expert", None, "dp"),
        P("expert", "dp", None),
        P("dp", "expert", None, None),
    )
    return jax.shard_map(
        shards,
        mesh=mesh,
        in_specs=placed,
        out_specs=(P("expert", "dp"), P("dp", "expert", None)),
        check_vma=False,
    )
```
